512 devices in a mesh: gy: 32 (over z, y_lo), gz: 16 (over x, y_hi, core).
Axes of the slice: x: 4, y: 8 (y_hi: 2, y_lo: 4; y = y_hi * 4 + y_lo), z: 8, core: 2. Of those that a mesh axis runs over, the one named last changes fastest.
Arguments:
- scalar: float32 [64, 768, 768], P('gz', 'gy'), may hold values from -6 to 6
- velocity: float32 [3, 64, 256, 256], P(None, None, 'gy', 'gz'), may hold values from -0.9 to 0.9
Outputs:
- remeshed: float32 [64, 768, 768], P('gz', 'gy')
The draws below stay inside these ranges and needn't reach their ends.
All inputs are finite; a program needn't handle non-finite values.
Results may differ from the reference program's by a relative error of at most 0.0003.
Values sent between devices are 32-bit elements; how exact they have to be, the bound alone decides.
A program may use at most 64 MiB of HBM per device.

```python
import jax
import jax.numpy as jnp
from jax import lax

NX = 768
NY = 768
NZ = 64
NXC = 256
NYC = 256


def level_of(stream_key, dims, cuts, smallest, high):
    factor_of = 1.0
    for position, shards_of in cuts:
        heights = jax.random.uniform(jax.random.fold_in(jax.random.fold_in(stream_key, 6), position), (shards_of,), jnp.float32, smallest / len(cuts), high / len(cuts))
        factor_of = factor_of * jnp.repeat(jnp.exp(heights), dims[position] // shards_of).reshape((-1,) + (1,) * (len(dims) - 1 - position))
    return factor_of


def bell_draw(stream_key, dims, scale, most, cuts=(), held_as=jnp.bfloat16):
    gain = level_of(stream_key, dims, cuts, -0.22, 0.18) if cuts else 1.0
    array = jax.random.normal(stream_key, dims, jnp.float32) * scale * gain
    return jnp.minimum(jnp.maximum(array, -most), most).astype(held_as)


def setup_inputs(seed: int = 0) -> dict:
    key_of = jax.random.split(jax.random.key(seed), 3)
    scalar = bell_draw(key_of[0], (NZ, NY, NX), 1.0, 6.0, ((0, 16), (1, 32)), jnp.float32)
    velocity = jnp.clip(jax.random.uniform(key_of[1], (3, NZ, NYC, NXC), jnp.float32, -0.9, 0.9) * level_of(key_of[1], (3, NZ, NYC, NXC), ((2, 32), (3, 16)), -0.4, 0.0), -0.9, 0.9)
    return {"scalar": scalar, "velocity": velocity}


def alternate(current, following, along):
    pieces = [current * (1.0 - phase / 3.0) + following * (phase / 3.0) for phase in range(3)]
    stacked = jnp.stack(pieces, axis=along + 1)
    new_shape = list(current.shape)
    new_shape[along] = new_shape[along] * 3
    return stacked.reshape(new_shape)


def polynomial(factors, value):
    result = jnp.zeros_like(value)
    for factor in reversed(factors):
        result = result * value + factor
    return result


def kernel_weight(offset):
    size = jnp.abs(offset)
    inner = polynomial([1.0, 0.0, -5.0 / 4.0, -35.0 / 12.0, 21.0 / 4.0, -25.0 / 12.0], size)
    middle = polynomial([-4.0, 75.0 / 4.0, -245.0 / 8.0, 545.0 / 24.0, -63.0 / 8.0, 25.0 / 24.0], size)
    outer = polynomial([18.0, -153.0 / 4.0, 255.0 / 8.0, -313.0 / 24.0, 21.0 / 8.0, -5.0 / 24.0], size)
    return jnp.where(size < 1.0, inner, jnp.where(size < 2.0, middle, jnp.where(size < 3.0, outer, 0.0)))


def displacement(speed, before, after):
    half_step = 0.5 * speed
    return jnp.where(half_step >= 0.0, (1.0 - half_step) * speed + half_step * after, (1.0 + half_step) * speed - half_step * before)


def sweep_periodic(field, speed, along):
    moved = displacement(speed, jnp.roll(speed, 1, along), jnp.roll(speed, -1, along))
    result = jnp.zeros_like(field)
    for offset in range(-3, 4):
        result = result + jnp.roll(field * kernel_weight(offset - moved), offset, along)
    return result


def sweep_open(field, speed):
    zero_plane = jnp.zeros_like(speed[:1])
    before = jnp.concatenate([zero_plane, speed[:-1]], axis=0)
    after = jnp.concatenate([speed[1:], zero_plane], axis=0)
    moved = displacement(speed, before, after)
    count = field.shape[0]
    total = jnp.zeros((count + 6,) + field.shape[1:], jnp.float32)
    for offset in range(-3, 4):
        total = total.at[3 + offset:3 + offset + count].add(field * kernel_weight(offset - moved))
    return total[3:3 + count]


def plane_sweeps(pair):
    plane, coarse = pair
    y_fine = alternate(coarse, jnp.roll(coarse, -1, 1), 1)
    fine_vel = alternate(y_fine, jnp.roll(y_fine, -1, 2), 2)
    field = sweep_periodic(plane, fine_vel[0], 1)
    field = sweep_periodic(field, fine_vel[1], 0)
    return field.T, fine_vel[2].T


def column_sweep(pair):
    return sweep_open(pair[0], pair[1])


def reference(scalar, velocity):
    swept, vertical = lax.map(plane_sweeps, (scalar, jnp.moveaxis(velocity, 1, 0)))
    columns = lax.map(column_sweep, (jnp.moveaxis(swept, 1, 0), jnp.moveaxis(vertical, 1, 0)))
    return jnp.moveaxis(columns, 0, 1)
```

```python
import functools

import jax
import jax.numpy as jnp
import numpy as np
from jax import lax
from jax.experimental import pallas as pl
from jax.experimental.pallas import tpu as pltpu
from jax.sharding import PartitionSpec as P

LANES = 128
INNER = [1.0, 0.0, -5.0 / 4.0, -35.0 / 12.0, 21.0 / 4.0, -25.0 / 12.0]
MIDDLE = [-4.0, 75.0 / 4.0, -245.0 / 8.0, 545.0 / 24.0, -63.0 / 8.0, 25.0 / 24.0]
OUTER = [18.0, -153.0 / 4.0, 255.0 / 8.0, -313.0 / 24.0, 21.0 / 8.0, -5.0 / 24.0]


def shifted(factors, base, slope):
    total = np.polynomial.Polynomial([0.0])
    for factor in reversed(factors):
        total = total * np.polynomial.Polynomial([base, slope]) + factor
    coefs = np.zeros(6)
    coefs[: len(total.coef)] = total.coef
    return [0.0 if abs(c) < 1e-10 else float(c) for c in coefs]


AHEAD = {1: shifted(INNER, 1.0, -1.0), 2: shifted(MIDDLE, 2.0, -1.0), 3: shifted(OUTER, 3.0, -1.0)}
BEHIND = {1: shifted(MIDDLE, 1.0, 1.0), 2: shifted(OUTER, 2.0, 1.0)}


def horner(factors, value):
    lowest = 0
    while factors[lowest] == 0.0:
        lowest += 1
    result = jnp.full_like(value, factors[-1])
    for factor in reversed(factors[lowest:-1]):
        result = result * value
        if factor != 0.0:
            result = result + factor
    for _ in range(lowest):
        result = result * value
    return result


def weights(moved):
    size = jnp.abs(moved)
    positive = moved >= 0.0
    result = {0: horner(INNER, size)}
    for m in (1, 2, 3):
        near = horner(AHEAD[m], size)
        far = horner(BEHIND[m], size) if m in BEHIND else jnp.zeros_like(size)
        result[m] = jnp.where(positive, near, far)
        result[-m] = jnp.where(positive, far, near)
    return result


def displacement(speed, before, after):
    return speed + 0.5 * speed * jnp.where(speed >= 0.0, after - speed, speed - before)


def roll(value, shift, axis):
    return pltpu.roll(value, shift % value.shape[axis], axis)


def sweep_periodic(field, speed, axis):
    moved = displacement(speed, roll(speed, 1, axis), roll(speed, -1, axis))
    w = weights(moved)
    result = field * w[0]
    for m in (-3, -2, -1, 1, 2, 3):
        result = result + roll(field * w[m], m, axis)
    return result


def split(value):
    high = value.astype(jnp.bfloat16)
    return high, (value - high.astype(jnp.float32)).astype(jnp.bfloat16)


def dot(a, b, dims=((1,), (0,))):
    return lax.dot_general(a, b, (dims, ((), ())), preferred_element_type=jnp.float32)


def exact_left(a, value, dims=((1,), (0,))):
    high, low = split(value)
    return dot(a, high, dims) + dot(a, low, dims)


def exact_right(value, b):
    high, low = split(value)
    return dot(high, b) + dot(low, b)


HALO = 3
GROUP = 32


def plan(nz, xc, bc, even):
    first = {True: (0, 0, 0), False: (bc - 1, bc, bc)}[even]
    last = {True: (bc + 2, bc + 1, bc + 1), False: (xc, xc, xc)}[even]
    return [(c, x, nz + (c == 2)) for c in range(3) for x in range(first[c], last[c])]


def side_plan(nz, xc):
    return [(0, xc - 1, nz), (0, 0, nz), (0, 1, nz), (1, 0, nz), (2, 0, nz + 1)]


def positions(entries):
    at, out = 0, []
    for c, x, n in entries:
        out.append((at, c, x, n))
        at += n
    assert at <= LANES
    return out


def constants(nz, gz, gy, yc, xc):
    bc = gz * xc // gy
    bf = 3 * bc
    ny = 3 * gy * yc
    to_xy = np.zeros((2, 2 * LANES, 2 * LANES), np.float32)
    to_z = np.zeros((2, (nz + 1) * bf, 2 * LANES), np.float32)
    for odd in range(2):
        where = {}
        for at, c, x, n in positions(plan(nz, xc, bc, not odd)):
            for i in range(n):
                where[c, x - odd * bc, i] = at + i
        for at, c, x, n in positions(side_plan(nz, xc)):
            col = x + xc - odd * bc if odd else x - xc
            if (c, col, 0) in where or (odd and x == xc - 1) or (not odd and x != xc - 1):
                continue
            for i in range(n):
                where[c, col, i] = LANES + at + i
        for c in range(3):
            reach = range(-HALO, bf + HALO) if c == 0 else range(bf)
            for col in reach:
                k = col % 3
                for rel, weight in ((col // 3, 3 - k), (col // 3 + 1, k)):
                    if weight == 0:
                        continue
                    for i in range(nz + (c == 2)):
                        src = where[c, rel, i]
                        if c == 0:
                            to_xy[odd, src, (GROUP * i + col) % LANES] += weight
                        elif c == 1:
                            to_xy[odd, src, LANES + GROUP * i + col] += weight
                        else:
                            to_z[odd, bf * i + col, src] += weight
    along = np.zeros((gy * yc, ny), np.float32)
    for c in range(gy * yc):
        for k in range(3):
            along[c, 3 * c + k] += 3 - k
            along[(c + 1) % (gy * yc), 3 * c + k] += k
    return to_xy, to_z, along, np.ascontiguousarray(along.T)


def wrapped(index, size):
    return jnp.where(index >= size, index - size, index)


def kernel(gz, gy, nz, yc, xc, *refs):
    (scalar_hbm, vel_hbm, xy_hbm, zz_hbm, ey_hbm, eyt_hbm, out,
     scalar, vel, xy_m, zz_m, ey_m, eyt_m,
     vsend, ssend, vmain, vside, blocks, pencil, edge_out, edge_in,
     up_out, down_out, up_in, down_in,
     local_sem, main_s, main_r, side_s, side_r, blk_s, blk_r, edge_s, z_s, z_r) = refs
    h = lax.axis_index("gz")
    s = lax.axis_index("gy")
    rf = 3 * yc
    bc = gz * xc // gy
    bf = 3 * bc
    total = gz * nz
    nx = scalar.shape[2]
    ny = gy * rf
    odd = lax.rem(s, 2)
    owner = lax.div(s, 2)
    beside = wrapped(owner + jnp.where(odd == 1, 1, gz - 1), gz)
    partner = h + 1 - 2 * lax.rem(h, 2)

    loads = []
    for i, (src, dst) in enumerate((
        (vel_hbm, vel), (scalar_hbm, scalar), (xy_hbm.at[odd], xy_m), (zz_hbm.at[odd], zz_m),
        (ey_hbm, ey_m), (eyt_hbm, eyt_m),
    )):
        load = pltpu.make_async_copy(src, dst, local_sem.at[i])
        load.start()
        loads.append(load)

    barrier = pltpu.get_barrier_semaphore()

    def greet(p, g):
        pl.semaphore_signal(
            barrier, inc=1, device_id={"gz": p, "gy": g}, device_id_type=pl.DeviceIdType.MESH
        )

    for step in range(1, gy):
        g = wrapped(s + step, gy)
        greet(h, g)
        greet(owner, g)
        greet(beside, g)

    @pl.when(owner != h)
    def _():
        greet(owner, s)

    @pl.when(beside != h)
    def _():
        greet(beside, s)

    @pl.when(h > 0)
    def _():
        greet(h - 1, s)

    @pl.when(h < gz - 1)
    def _():
        greet(h + 1, s)

    own = (owner == h).astype(jnp.int32) + (beside == h).astype(jnp.int32)
    ends = (h == 0).astype(jnp.int32) + (h == gz - 1).astype(jnp.int32)

    def remote(src, dst, send, recv, p, g):
        return pltpu.make_async_remote_copy(
            src_ref=src, dst_ref=dst, send_sem=send, recv_sem=recv,
            device_id={"gz": p, "gy": g}, device_id_type=pl.DeviceIdType.MESH,
        )

    loads[0].wait()
    lane = lax.broadcasted_iota(jnp.int32, (yc, LANES), 1)
    row = lax.broadcasted_iota(jnp.int32, (yc, LANES), 0)
    fill = jnp.zeros((yc, LANES - total), jnp.float32)
    source = {
        (c, x): jnp.concatenate([vel[c, :, x, :], fill], axis=1)
        for c in range(3) for x in range(xc)
    }

    def message(entries, p):
        tile = jnp.zeros((yc, LANES), jnp.float32)
        for at, c, x, n in positions(entries):
            z = p * nz - (1 - p % 2 if c == 2 else 0)
            tile = jnp.where(
                (lane >= at) & (lane < at + n), roll(source[c, x], at - z, 1), tile
            )
        return tile

    parts = LANES // GROUP
    for p in range(gz):
        vsend[p, 0] = message(plan(nz, xc, bc, True), p)
        vsend[p, 1] = message(plan(nz, xc, bc, False), p)
        tile = message(side_plan(nz, xc), p)
        wide = tile
        for k in range(1, parts):
            wide = jnp.where(row % parts == k, roll(tile, k * GROUP, 1), wide)
        ssend[p] = jnp.concatenate(
            [jnp.sum(wide[i : i + parts], axis=0, keepdims=True) for i in range(0, yc, parts)],
            axis=0,
        )

    pl.semaphore_wait(barrier, 3 * (gy - 1) + 4 - own - ends)

    def main_copy(p, c, act, own_too):
        g = 2 * h + c
        mine = (p == h) & (g == s)

        @pl.when(jnp.logical_not(mine))
        def _():
            act(remote(vsend.at[p, c], vmain.at[s], main_s.at[2 * p + c], main_r.at[s], p, g))

        if own_too:
            @pl.when(mine)
            def _():
                act(pltpu.make_async_copy(vsend.at[p, c], vmain.at[s], main_r.at[s]))

    def side_copy(p, c, act, own_too):
        g = wrapped(2 * h + (2 if c else gy - 1), gy)
        mine = (p == h) & (g == s)

        @pl.when(jnp.logical_not(mine))
        def _():
            act(remote(ssend.at[p], vside.at[s], side_s.at[2 * p + c], side_r.at[s], p, g))

        if own_too:
            @pl.when(mine)
            def _():
                act(pltpu.make_async_copy(ssend.at[p], vside.at[s], side_r.at[s]))

    tiles = [(p, c) for p in range(gz) for c in range(2)]
    for p, c in tiles:
        main_copy(p, c, lambda copy: copy.start(), True)
    for p, c in tiles:
        side_copy(p, c, lambda copy: copy.start(), True)

    loads[1].wait()
    wide = lax.broadcasted_iota(jnp.int32, (rf, LANES), 1)
    place = [lax.rem(wide + (HALO - GROUP * z) % LANES, LANES) for z in range(nz)]
    for g in range(gy):
        low = g * bf - HALO
        tile = jnp.zeros((rf, LANES), jnp.float32)
        for z in range(nz):
            for t in range(low // LANES, (low + GROUP - 1) // LANES + 1):
                at = t * LANES % nx
                piece = scalar[z, :, at : at + LANES]
                begin = max(0, t * LANES - low)
                end = min(GROUP, (t + 1) * LANES - low)
                tile = jnp.where(
                    (place[z] >= begin) & (place[z] < end),
                    roll(piece, z * GROUP - g * bf, 1),
                    tile,
                )
        blocks[g] = tile

    def block_copy(step):
        g = wrapped(s + step, gy)
        if step == 0:
            return pltpu.make_async_copy(blocks.at[g], pencil.at[s], blk_r.at[s])
        return remote(blocks.at[g], pencil.at[s], blk_s.at[step], blk_r.at[s], h, g)

    sends = [block_copy(step) for step in range(gy)]
    for copy in sends[1:] + sends[:1]:
        copy.start()

    for load in loads[2:]:
        load.wait()
    for i in range(gy):
        pltpu.make_async_copy(vmain.at[i], vmain.at[i], main_r.at[i]).wait()
        pltpu.make_async_copy(vside.at[i], vside.at[i], side_r.at[i]).wait()

    sides = []
    for i in range(gy):
        both = vside[i]
        tall = jnp.where(row < parts, both[0:1], both[1:2])
        tile = tall
        for k in range(1, parts):
            tile = jnp.where(row % parts == k, roll(tall, -k * GROUP, 1), tile)
        sides.append(tile)
    nyc = gy * yc
    coarse = jnp.concatenate(
        [vmain[...].reshape(nyc, LANES), jnp.concatenate(sides, axis=0)], axis=1
    )
    ninth = 1.0 / 9.0
    speed = exact_left(eyt_m[...], exact_right(coarse, xy_m[...])) * ninth
    speed_z = exact_right(exact_left(zz_m[...], coarse, ((1,), (1,))), ey_m[...]) * ninth

    upper = lax.rem(h, 2) == 1
    edge_out[...] = jnp.where(upper, speed_z[:bf], speed_z[nz * bf :])
    edge = remote(edge_out, edge_in, edge_s.at[0], edge_s.at[1], partner, s)
    edge.start()

    for i in range(gy):
        pltpu.make_async_copy(pencil.at[i], pencil.at[i], blk_r.at[i]).wait()
    field = pencil[...].reshape(ny, LANES)
    field = sweep_periodic(field, speed[:, :LANES], 1)
    field = sweep_periodic(field, speed[:, LANES:], 0)

    edge.wait()
    chunks = ny // LANES
    below, above = wrapped(h + gz - 1, gz), wrapped(h + 1, gz)
    ups, downs = [], []
    for k in range(chunks):
        cols = slice(k * LANES, (k + 1) * LANES)
        turned = jnp.transpose(field[cols])
        part = jnp.concatenate([turned[GROUP * z : GROUP * z + bf] for z in range(nz)], axis=0)
        near, far = speed_z[:, cols], edge_in[:, cols]
        six = jnp.concatenate(
            [jnp.where(upper, far, near[:bf]),
             jnp.where(upper, near[: nz * bf], near[bf:]),
             jnp.where(upper, near[nz * bf :], far)], axis=0
        )
        moved = displacement(
            six[bf : (nz + 1) * bf], six[: nz * bf], six[2 * bf :]
        )
        w = weights(moved)

        def landing(target):
            result = None
            for m in range(-3, 4):
                z = target - m
                if 0 <= z < nz:
                    at = slice(z * bf, (z + 1) * bf)
                    term = part[at] * w[m][at]
                    result = term if result is None else result + term
            return result

        for i in range(3):
            up_out[k, i] = landing(nz + i)
            down_out[k, i] = landing(i - 3)
        up = remote(up_out.at[k], up_in.at[k], z_s.at[0, k], z_r.at[0, k], above, s)
        down = remote(down_out.at[k], down_in.at[k], z_s.at[1, k], z_r.at[1, k], below, s)
        ups.append(up)
        downs.append(down)

        @pl.when(h < gz - 1)
        def _():
            up.start()

        @pl.when(h > 0)
        def _():
            down.start()

        for i in range(nz):
            out[i, :, cols] = landing(i)

    @pl.when(h > 0)
    def _():
        for k in range(chunks):
            cols = slice(k * LANES, (k + 1) * LANES)
            ups[k].wait_recv()
            for i in range(3):
                out[i, :, cols] = out[i, :, cols] + up_in[k, i]
        for copy in downs:
            copy.wait_send()

    @pl.when(h < gz - 1)
    def _():
        for k in range(chunks):
            cols = slice(k * LANES, (k + 1) * LANES)
            downs[k].wait_recv()
            for i in range(nz - 3, nz):
                out[i, :, cols] = out[i, :, cols] + down_in[k, i - nz + 3]
        for copy in ups:
            copy.wait_send()

    for copy in sends[1:]:
        copy.wait_send()
    for p, c in tiles:
        main_copy(p, c, lambda copy: copy.wait_send(), False)
        side_copy(p, c, lambda copy: copy.wait_send(), False)


def local(scalar, velocity):
    gz, gy = lax.axis_size("gz"), lax.axis_size("gy")
    nz, rf, nx = scalar.shape
    yc, xc = velocity.shape[2:]
    bc = gz * xc // gy
    bf = 3 * bc
    ny = gy * rf
    mats = [jnp.asarray(m, jnp.bfloat16) for m in constants(nz, gz, gy, yc, xc)]
    turned = jnp.transpose(velocity, (0, 2, 3, 1))
    f32 = jnp.float32
    dma = pltpu.SemaphoreType.DMA
    anywhere = pl.BlockSpec(memory_space=pl.ANY)
    vmem = pl.BlockSpec(memory_space=pltpu.VMEM)
    scratch = [pltpu.VMEM(scalar.shape, f32), pltpu.VMEM(turned.shape, f32)]
    scratch += [pltpu.VMEM(m.shape[1:], jnp.bfloat16) for m in mats[:2]]
    scratch += [pltpu.VMEM(m.shape, jnp.bfloat16) for m in mats[2:]]
    scratch += [
        pltpu.VMEM((gz, 2, yc, LANES), f32),
        pltpu.VMEM((gz, 2, LANES), f32),
        pltpu.VMEM((gy, yc, LANES), f32),
        pltpu.VMEM((gy, 2, LANES), f32),
        pltpu.VMEM((gy, rf, LANES), f32),
        pltpu.VMEM((gy, rf, LANES), f32),
        pltpu.VMEM((bf, ny), f32),
        pltpu.VMEM((bf, ny), f32),
    ]
    scratch += [pltpu.VMEM((ny // LANES, 3, bf, LANES), f32)] * 4
    scratch += [dma((n,)) for n in (2 + len(mats), 2 * gz, gy, 2 * gz, gy, gy, gy, 2)]
    scratch += [dma((2, ny // LANES))] * 2
    return pl.pallas_call(
        functools.partial(kernel, gz, gy, nz, yc, xc),
        out_shape=pltpu.VMEM((nz, bf, ny), f32),
        in_specs=[anywhere] * (2 + len(mats)),
        out_specs=vmem,
        scratch_shapes=scratch,
        compiler_params=pltpu.CompilerParams(has_side_effects=True, collective_id=0),
    )(scalar, turned, *mats)


def solution(mesh):
    in_specs = (P("gz", "gy", None), P(None, None, "gy", "gz"))
    out_specs = P("gz", "gy", None)
    return jax.shard_map(local, mesh=mesh, in_specs=in_specs, out_specs=out_specs, check_vma=False)
```

```python
import functools

import jax
import jax.numpy as jnp
import numpy as np
from jax import lax
from jax.experimental import pallas as pl
from jax.experimental.pallas import tpu as pltpu
from jax.sharding import PartitionSpec as P

LANES = 128
INNER = [1.0, 0.0, -5.0 / 4.0, -35.0 / 12.0, 21.0 / 4.0, -25.0 / 12.0]
MIDDLE = [-4.0, 75.0 / 4.0, -245.0 / 8.0, 545.0 / 24.0, -63.0 / 8.0, 25.0 / 24.0]
OUTER = [18.0, -153.0 / 4.0, 255.0 / 8.0, -313.0 / 24.0, 21.0 / 8.0, -5.0 / 24.0]


def shifted(factors, base, slope):
    total = np.polynomial.Polynomial([0.0])
    for factor in reversed(factors):
        total = total * np.polynomial.Polynomial([base, slope]) + factor
    coefs = np.zeros(6)
    coefs[: len(total.coef)] = total.coef
    return [0.0 if abs(c) < 1e-10 else float(c) for c in coefs]


AHEAD = {1: shifted(INNER, 1.0, -1.0), 2: shifted(MIDDLE, 2.0, -1.0), 3: shifted(OUTER, 3.0, -1.0)}
BEHIND = {1: shifted(MIDDLE, 1.0, 1.0), 2: shifted(OUTER, 2.0, 1.0)}


def horner(factors, value):
    lowest = 0
    while factors[lowest] == 0.0:
        lowest += 1
    result = jnp.full_like(value, factors[-1])
    for factor in reversed(factors[lowest:-1]):
        result = result * value
        if factor != 0.0:
            result = result + factor
    for _ in range(lowest):
        result = result * value
    return result


def weights(moved):
    size = jnp.abs(moved)
    positive = moved >= 0.0
    result = {0: horner(INNER, size)}
    for m in (1, 2, 3):
        near = horner(AHEAD[m], size)
        far = horner(BEHIND[m], size) if m in BEHIND else jnp.zeros_like(size)
        result[m] = jnp.where(positive, near, far)
        result[-m] = jnp.where(positive, far, near)
    return result


def displacement(speed, before, after):
    return speed + 0.5 * speed * jnp.where(speed >= 0.0, after - speed, speed - before)


def roll(value, shift, axis):
    return pltpu.roll(value, shift % value.shape[axis], axis)


def sweep_periodic(field, speed, axis):
    moved = displacement(speed, roll(speed, 1, axis), roll(speed, -1, axis))
    w = weights(moved)
    result = field * w[0]
    for m in (-3, -2, -1, 1, 2, 3):
        result = result + roll(field * w[m], m, axis)
    return result


def split(value):
    high = value.astype(jnp.bfloat16)
    return high, (value - high.astype(jnp.float32)).astype(jnp.bfloat16)


def dot(a, b, dims=((1,), (0,))):
    return lax.dot_general(a, b, (dims, ((), ())), preferred_element_type=jnp.float32)


def exact_left(a, value, dims=((1,), (0,))):
    high, low = split(value)
    return dot(a, high, dims) + dot(a, low, dims)


def exact_right(value, b):
    high, low = split(value)
    return dot(high, b) + dot(low, b)


HALO = 3
EDGE = 8
GROUP = 32


def plan(nz, xc, bc, even):
    first = {True: (0, 0, 0), False: (bc - 1, bc, bc)}[even]
    last = {True: (bc + 2, bc + 1, bc + 1), False: (xc, xc, xc)}[even]
    return [(c, x, nz + (c == 2)) for c in range(3) for x in range(first[c], last[c])]


def side_plan(nz, xc):
    return [(0, xc - 1, nz), (0, 0, nz), (0, 1, nz), (1, 0, nz), (2, 0, nz + 1)]


def positions(entries):
    at, out = 0, []
    for c, x, n in entries:
        out.append((at, c, x, n))
        at += n
    assert at <= LANES
    return out


def constants(nz, gz, gy, yc, xc):
    bc = gz * xc // gy
    bf = 3 * bc
    ny = 3 * gy * yc
    to_xy = np.zeros((2, 2 * LANES, 2 * LANES), np.float32)
    to_z = np.zeros((2, (nz + 1) * bf, 2 * LANES), np.float32)
    for odd in range(2):
        where = {}
        for at, c, x, n in positions(plan(nz, xc, bc, not odd)):
            for i in range(n):
                where[c, x - odd * bc, i] = at + i
        for at, c, x, n in positions(side_plan(nz, xc)):
            col = x + xc - odd * bc if odd else x - xc
            if (c, col, 0) in where or (odd and x == xc - 1) or (not odd and x != xc - 1):
                continue
            for i in range(n):
                where[c, col, i] = LANES + at + i
        for c in range(3):
            reach = range(-HALO, bf + HALO) if c == 0 else range(bf)
            for col in reach:
                k = col % 3
                for rel, weight in ((col // 3, 3 - k), (col // 3 + 1, k)):
                    if weight == 0:
                        continue
                    for i in range(nz + (c == 2)):
                        src = where[c, rel, i]
                        if c == 0:
                            to_xy[odd, src, (GROUP * i + col) % LANES] += weight
                        elif c == 1:
                            to_xy[odd, src, LANES + GROUP * i + col] += weight
                        else:
                            to_z[odd, bf * i + col, src] += weight
    along = np.zeros((gy * yc, ny), np.float32)
    for c in range(gy * yc):
        for k in range(3):
            along[c, 3 * c + k] += 3 - k
            along[(c + 1) % (gy * yc), 3 * c + k] += k
    return to_xy, to_z, along, np.ascontiguousarray(along.T)


def wrapped(index, size):
    return jnp.where(index >= size, index - size, index)


def kernel(gz, gy, nz, yc, xc, *refs):
    (scalar_hbm, vel_hbm, xy_hbm, zz_hbm, ey_hbm, eyt_hbm, out,
     scalar, vel, xy_m, zz_m, ey_m, eyt_m,
     vsend, ssend, vmain, vside, blocks, pencil, after, speed_y, turned_z, edge_out, edge_in,
     up_out, down_out, up_in, down_in,
     local_sem, main_s, main_r, side_s, side_r, blk_s, blk_r, edge_s, z_s, z_r,
     ready_b, ready_v, ready_z) = refs
    h = lax.axis_index("gz")
    s = lax.axis_index("gy")
    rf = 3 * yc
    bc = gz * xc // gy
    bf = 3 * bc
    total = gz * nz
    nx = scalar.shape[2]
    ny = gy * rf
    odd = lax.rem(s, 2)
    owner = lax.div(s, 2)
    beside = wrapped(owner + jnp.where(odd == 1, 1, gz - 1), gz)
    partner = h + 1 - 2 * lax.rem(h, 2)

    loads = []
    for i, (src, dst) in enumerate((
        (vel_hbm, vel), (scalar_hbm, scalar), (xy_hbm.at[odd], xy_m), (zz_hbm.at[odd], zz_m),
        (ey_hbm, ey_m), (eyt_hbm, eyt_m),
    )):
        load = pltpu.make_async_copy(src, dst, local_sem.at[i])
        load.start()
        loads.append(load)

    barrier = pltpu.get_barrier_semaphore()

    def greet(p, g):
        pl.semaphore_signal(
            barrier, inc=1, device_id={"gz": p, "gy": g}, device_id_type=pl.DeviceIdType.MESH
        )

    def flag(condition):
        return jnp.where(condition, 1, 0)

    reach = [wrapped(2 * h + (j - 1 if j else gy - 1), gy) for j in range(4)]

    def greet_higher(g, _):
        greet(h, g)
        greet(owner, g)
        greet(beside, g)
        return 0

    lax.fori_loop(s + 1, gy, greet_higher, 0)

    def higher_targets(g, act):
        def one(q, _):
            act(q)
            return 0

        lax.fori_loop(jnp.where(g > s, 0, jnp.where(g == s, h + 1, gz)), gz, one, 0)

    for g in reach:
        higher_targets(g, lambda q, g=g: greet(q, g))

    @pl.when(owner > h)
    def _():
        greet(owner, s)

    @pl.when(beside > h)
    def _():
        greet(beside, s)

    @pl.when(h < gz - 1)
    def _():
        greet(h + 1, s)

    lower = 3 * s + flag(owner < h) + flag(beside < h) + flag(h > 0)
    for g in reach:
        lower = lower + jnp.where(g < s, gz, jnp.where(g == s, h, 0))

    @pl.when(lower > 0)
    def _():
        pl.semaphore_wait(barrier, lower)

    def tell(semaphore, p, g):
        pl.semaphore_signal(
            semaphore, inc=1, device_id={"gz": p, "gy": g}, device_id_type=pl.DeviceIdType.MESH
        )

    from_owner = ready_v.at[4 * h + 1 + odd]
    from_beside = ready_v.at[4 * h + 3 - 3 * odd]

    def tell_lower(g, _):
        tell(ready_b.at[s], h, g)
        tell(from_owner, owner, g)
        tell(from_beside, beside, g)
        return 0

    lax.fori_loop(0, s, tell_lower, 0)

    @pl.when(owner < h)
    def _():
        tell(from_owner, owner, s)

    @pl.when(beside < h)
    def _():
        tell(from_beside, beside, s)

    @pl.when(h > 0)
    def _():
        tell(ready_z, h - 1, s)

    def remote(src, dst, send, recv, p, g):
        return pltpu.make_async_remote_copy(
            src_ref=src, dst_ref=dst, send_sem=send, recv_sem=recv,
            device_id={"gz": p, "gy": g}, device_id_type=pl.DeviceIdType.MESH,
        )

    loads[0].wait()
    lane = lax.broadcasted_iota(jnp.int32, (yc, LANES), 1)
    row = lax.broadcasted_iota(jnp.int32, (yc, LANES), 0)
    fill = jnp.zeros((yc, LANES - total), jnp.float32)
    source = {
        (c, x): jnp.concatenate([vel[c, :, x, :], fill], axis=1)
        for c in range(3) for x in range(xc)
    }

    def message(entries, p):
        tile = jnp.zeros((yc, LANES), jnp.float32)
        for at, c, x, n in positions(entries):
            z = p * nz - (1 - p % 2 if c == 2 else 0)
            tile = jnp.where(lane >= at, roll(source[c, x], at - z, 1), tile)
        return jnp.where(lane < at + n, tile, 0.0)

    parts = LANES // GROUP
    for p in range(gz):
        vsend[p, 0] = message(plan(nz, xc, bc, True), p)
        vsend[p, 1] = message(plan(nz, xc, bc, False), p)
        tile = message(side_plan(nz, xc), p)
        wide = tile
        for k in range(1, parts):
            wide = jnp.where(row % parts == k, roll(tile, k * GROUP, 1), wide)
        ssend[p] = jnp.concatenate(
            [jnp.sum(wide[i : i + parts], axis=0, keepdims=True) for i in range(0, yc, parts)],
            axis=0,
        )

    def main_copy(p, c, act, own_too):
        g = 2 * h + c
        mine = (p == h) & (g == s)

        @pl.when(jnp.logical_not(mine))
        def _():
            act(remote(vsend.at[p, c], vmain.at[s], main_s.at[2 * p + c], main_r.at[s], p, g))

        if own_too:
            @pl.when(mine)
            def _():
                act(pltpu.make_async_copy(vsend.at[p, c], vmain.at[s], main_r.at[s]))

    def side_copy(p, c, act, own_too):
        g = wrapped(2 * h + (2 if c else gy - 1), gy)
        mine = (p == h) & (g == s)

        @pl.when(jnp.logical_not(mine))
        def _():
            act(remote(ssend.at[p], vside.at[s], side_s.at[2 * p + c], side_r.at[s], p, g))

        if own_too:
            @pl.when(mine)
            def _():
                act(pltpu.make_async_copy(ssend.at[p], vside.at[s], side_r.at[s]))

    tiles = [(p, c) for p in range(gz) for c in range(2)]

    def send_velocity():
        for j in (1, 2, 0, 3):
            higher_targets(reach[j], lambda q, j=j: pl.semaphore_wait(ready_v.at[4 * q + j], 1))
            for p in range(gz):
                (main_copy if j in (1, 2) else side_copy)(
                    p, j - 1 if j in (1, 2) else j // 3, lambda copy: copy.start(), True
                )

    soon = 2 * h + 1 < s

    @pl.when(soon)
    def _():
        send_velocity()

    loads[1].wait()
    wide = lax.broadcasted_iota(jnp.int32, (rf, LANES), 1)
    place = [lax.rem(wide + (HALO - GROUP * z) % LANES, LANES) for z in range(nz)]
    for g in range(gy):
        low = g * bf - HALO
        tile = jnp.zeros((rf, LANES), jnp.float32)
        for z in range(nz):
            for t in range(low // LANES, (low + GROUP - 1) // LANES + 1):
                at = t * LANES % nx
                piece = scalar[z, :, at : at + LANES]
                begin = max(0, t * LANES - low)
                end = min(GROUP, (t + 1) * LANES - low)
                tile = jnp.where(
                    (place[z] >= begin) & (place[z] < end),
                    roll(piece, z * GROUP - g * bf, 1),
                    tile,
                )
        blocks[g] = tile

    def block_copy(step):
        g = jnp.where(step <= s, s - step, step)
        if step == 0:
            return pltpu.make_async_copy(blocks.at[g], pencil.at[s], blk_r.at[s])
        return remote(blocks.at[g], pencil.at[s], blk_s.at[step], blk_r.at[s], h, g)

    sends = [block_copy(step) for step in range(gy)]
    sends[0].start()
    for step in range(1, gy):
        @pl.when(step > s)
        def _():
            pl.semaphore_wait(ready_b.at[step], 1)

        sends[step].start()

    @pl.when(jnp.logical_not(soon))
    def _():
        send_velocity()

    for load in loads[2:]:
        load.wait()
    for i in range(gy):
        pltpu.make_async_copy(vmain.at[i], vmain.at[i], main_r.at[i]).wait()
        pltpu.make_async_copy(vside.at[i], vside.at[i], side_r.at[i]).wait()

    sides = []
    for i in range(gy):
        both = vside[i]
        tall = jnp.where(row < parts, both[0:1], both[1:2])
        tile = tall
        for k in range(1, parts):
            tile = jnp.where(row % parts == k, roll(tall, -k * GROUP, 1), tile)
        sides.append(tile)
    nyc = gy * yc
    coarse = jnp.concatenate(
        [vmain[...].reshape(nyc, LANES), jnp.concatenate(sides, axis=0)], axis=1
    )
    ninth = 1.0 / 9.0
    speed = exact_left(eyt_m[...], exact_right(coarse, xy_m[...])) * ninth
    speed_y[EDGE : EDGE + ny] = speed[:, LANES:]
    speed_y[:EDGE] = speed[ny - EDGE :, LANES:]
    speed_y[EDGE + ny :] = speed[:EDGE, LANES:]
    turned_z[...] = exact_right(exact_left(zz_m[...], coarse, ((1,), (1,))), ey_m[...]) * ninth

    upper = lax.rem(h, 2) == 1
    edge_out[...] = jnp.where(upper, turned_z[:bf], turned_z[nz * bf :])
    edge = remote(edge_out, edge_in, edge_s.at[0], edge_s.at[1], partner, s)

    @pl.when(h < gz - 1)
    def _():
        pl.semaphore_wait(ready_z, 1)

    edge.start()

    for i in range(gy):
        pltpu.make_async_copy(pencil.at[i], pencil.at[i], blk_r.at[i]).wait()
    joined = 4
    for i in range(0, gy, joined):
        rows = slice(i * rf, (i + joined) * rf)
        field = pencil[i : i + joined].reshape(joined * rf, LANES)
        after[EDGE + i * rf : EDGE + (i + joined) * rf] = sweep_periodic(
            field, speed[rows, :LANES], 1
        )
    after[:EDGE] = after[ny : ny + EDGE]
    after[EDGE + ny :] = after[EDGE : 2 * EDGE]

    edge.wait()
    chunks = ny // LANES
    below, above = wrapped(h + gz - 1, gz), wrapped(h + 1, gz)
    ups, downs = [], []
    for k in range(chunks):
        cols = slice(k * LANES, (k + 1) * LANES)
        rows = slice(k * LANES, (k + 1) * LANES + 2 * EDGE)
        swept = sweep_periodic(after[rows], speed_y[rows], 0)
        turned = jnp.transpose(swept[EDGE : EDGE + LANES])
        part = jnp.concatenate([turned[GROUP * z : GROUP * z + bf] for z in range(nz)], axis=0)
        near, far = turned_z[:, cols], edge_in[:, cols]
        six = jnp.concatenate(
            [jnp.where(upper, far, near[:bf]),
             jnp.where(upper, near[: nz * bf], near[bf:]),
             jnp.where(upper, near[nz * bf :], far)], axis=0
        )
        moved = displacement(
            six[bf : (nz + 1) * bf], six[: nz * bf], six[2 * bf :]
        )
        w = weights(moved)

        def landing(target):
            result = None
            for m in range(-3, 4):
                z = target - m
                if 0 <= z < nz:
                    at = slice(z * bf, (z + 1) * bf)
                    term = part[at] * w[m][at]
                    result = term if result is None else result + term
            return result

        for i in range(3):
            up_out[k, i] = landing(nz + i)
            down_out[k, i] = landing(i - 3)
        up = remote(up_out.at[k], up_in.at[k], z_s.at[0, k], z_r.at[0, k], above, s)
        down = remote(down_out.at[k], down_in.at[k], z_s.at[1, k], z_r.at[1, k], below, s)
        ups.append(up)
        downs.append(down)

        @pl.when(h < gz - 1)
        def _():
            up.start()

        @pl.when(h > 0)
        def _():
            down.start()

        for i in range(nz):
            out[i, :, cols] = landing(i)

    @pl.when(h > 0)
    def _():
        for k in range(chunks):
            cols = slice(k * LANES, (k + 1) * LANES)
            ups[k].wait_recv()
            for i in range(3):
                out[i, :, cols] = out[i, :, cols] + up_in[k, i]
        for copy in downs:
            copy.wait_send()

    @pl.when(h < gz - 1)
    def _():
        for k in range(chunks):
            cols = slice(k * LANES, (k + 1) * LANES)
            downs[k].wait_recv()
            for i in range(nz - 3, nz):
                out[i, :, cols] = out[i, :, cols] + down_in[k, i - nz + 3]
        for copy in ups:
            copy.wait_send()

    for copy in sends[1:]:
        copy.wait_send()
    for p, c in tiles:
        main_copy(p, c, lambda copy: copy.wait_send(), False)
        side_copy(p, c, lambda copy: copy.wait_send(), False)


def local(scalar, velocity):
    gz, gy = lax.axis_size("gz"), lax.axis_size("gy")
    nz, rf, nx = scalar.shape
    yc, xc = velocity.shape[2:]
    bc = gz * xc // gy
    bf = 3 * bc
    ny = gy * rf
    mats = [jnp.asarray(m, jnp.bfloat16) for m in constants(nz, gz, gy, yc, xc)]
    turned = jnp.transpose(velocity, (0, 2, 3, 1))
    f32 = jnp.float32
    dma = pltpu.SemaphoreType.DMA
    anywhere = pl.BlockSpec(memory_space=pl.ANY)
    vmem = pl.BlockSpec(memory_space=pltpu.VMEM)
    scratch = [pltpu.VMEM(scalar.shape, f32), pltpu.VMEM(turned.shape, f32)]
    scratch += [pltpu.VMEM(m.shape[1:], jnp.bfloat16) for m in mats[:2]]
    scratch += [pltpu.VMEM(m.shape, jnp.bfloat16) for m in mats[2:]]
    scratch += [
        pltpu.VMEM((gz, 2, yc, LANES), f32),
        pltpu.VMEM((gz, 2, LANES), f32),
        pltpu.VMEM((gy, yc, LANES), f32),
        pltpu.VMEM((gy, 2, LANES), f32),
        pltpu.VMEM((gy, rf, LANES), f32),
        pltpu.VMEM((gy, rf, LANES), f32),
        pltpu.VMEM((ny + 2 * EDGE, LANES), f32),
        pltpu.VMEM((ny + 2 * EDGE, LANES), f32),
        pltpu.VMEM(((nz + 1) * bf, ny), f32),
        pltpu.VMEM((bf, ny), f32),
        pltpu.VMEM((bf, ny), f32),
    ]
    scratch += [pltpu.VMEM((ny // LANES, 3, bf, LANES), f32)] * 4
    scratch += [dma((n,)) for n in (2 + len(mats), 2 * gz, gy, 2 * gz, gy, gy, gy, 2)]
    scratch += [dma((2, ny // LANES))] * 2
    regular = pltpu.SemaphoreType.REGULAR
    scratch += [regular((gy,)), regular((4 * gz,)), regular]
    return pl.pallas_call(
        functools.partial(kernel, gz, gy, nz, yc, xc),
        out_shape=pltpu.VMEM((nz, bf, ny), f32),
        in_specs=[anywhere] * (2 + len(mats)),
        out_specs=vmem,
        scratch_shapes=scratch,
        compiler_params=pltpu.CompilerParams(has_side_effects=True, collective_id=0),
    )(scalar, turned, *mats)


def solution(mesh):
    in_specs = (P("gz", "gy", None), P(None, None, "gy", "gz"))
    out_specs = P("gz", "gy", None)
    return jax.shard_map(local, mesh=mesh, in_specs=in_specs, out_specs=out_specs, check_vma=False)
```

```python
import functools

import jax
import jax.numpy as jnp
import numpy as np
from jax import lax
from jax.experimental import pallas as pl
from jax.experimental.pallas import tpu as pltpu
from jax.sharding import PartitionSpec as P

LANES = 128
INNER = [1.0, 0.0, -5.0 / 4.0, -35.0 / 12.0, 21.0 / 4.0, -25.0 / 12.0]
MIDDLE = [-4.0, 75.0 / 4.0, -245.0 / 8.0, 545.0 / 24.0, -63.0 / 8.0, 25.0 / 24.0]
OUTER = [18.0, -153.0 / 4.0, 255.0 / 8.0, -313.0 / 24.0, 21.0 / 8.0, -5.0 / 24.0]


def shifted(factors, base, slope):
    total = np.polynomial.Polynomial([0.0])
    for factor in reversed(factors):
        total = total * np.polynomial.Polynomial([base, slope]) + factor
    coefs = np.zeros(6)
    coefs[: len(total.coef)] = total.coef
    return [0.0 if abs(c) < 1e-10 else float(c) for c in coefs]


AHEAD = {1: shifted(INNER, 1.0, -1.0), 2: shifted(MIDDLE, 2.0, -1.0), 3: shifted(OUTER, 3.0, -1.0)}
BEHIND = {1: shifted(MIDDLE, 1.0, 1.0), 2: shifted(OUTER, 2.0, 1.0)}


def horner(factors, value):
    lowest = 0
    while factors[lowest] == 0.0:
        lowest += 1
    result = jnp.full_like(value, factors[-1])
    for factor in reversed(factors[lowest:-1]):
        result = result * value
        if factor != 0.0:
            result = result + factor
    for _ in range(lowest):
        result = result * value
    return result


def weights(moved):
    size = jnp.abs(moved)
    positive = moved >= 0.0
    result = {0: horner(INNER, size)}
    for m in (1, 2, 3):
        near = horner(AHEAD[m], size)
        far = horner(BEHIND[m], size) if m in BEHIND else jnp.zeros_like(size)
        result[m] = jnp.where(positive, near, far)
        result[-m] = jnp.where(positive, far, near)
    return result


def displacement(speed, before, after):
    return speed + 0.5 * speed * jnp.where(speed >= 0.0, after - speed, speed - before)


def roll(value, shift, axis):
    return pltpu.roll(value, shift % value.shape[axis], axis)


def sweep_periodic(field, speed, axis):
    moved = displacement(speed, roll(speed, 1, axis), roll(speed, -1, axis))
    w = weights(moved)
    result = field * w[0]
    for m in (-3, -2, -1, 1, 2, 3):
        result = result + roll(field * w[m], m, axis)
    return result


def split(value):
    high = value.astype(jnp.bfloat16)
    return high, (value - high.astype(jnp.float32)).astype(jnp.bfloat16)


def dot(a, b, dims=((1,), (0,))):
    return lax.dot_general(a, b, (dims, ((), ())), preferred_element_type=jnp.float32)


def exact_left(a, value, dims=((1,), (0,))):
    high, low = split(value)
    return dot(a, high, dims) + dot(a, low, dims)


def exact_right(value, b):
    high, low = split(value)
    return dot(high, b) + dot(low, b)


EDGE = 8
NINTH = 1.0 / 9.0


def along(count):
    out = np.zeros((count, 3 * count), np.float32)
    for c in range(count):
        for k in range(3):
            out[c, 3 * c + k] += 3 - k
            out[(c + 1) % count, 3 * c + k] += k
    return out


def constants(nz, gz, gy, yc, xc):
    bc = gz * xc // gy
    bf = 3 * bc
    rf = 3 * yc
    spare = LANES - nz * bf
    rows = np.zeros((nz * rf, nz * yc + 8), np.float32)
    for z in range(nz):
        for r in range(rf):
            y, k = divmod(r, 3)
            rows[z * rf + r, z * yc + y] += 3 - k
            rows[z * rf + r, z * yc + y + 1 if y < yc - 1 else nz * yc + z] += k
    groups = rf // yc
    to_y = np.zeros((groups * LANES, LANES), np.float32)
    to_z = np.zeros(((nz + 2) * bf, groups * LANES), np.float32)
    for plane in range(2 * nz + 2):
        for c in range(bf):
            for col, weight in ((c // 3, 3 - c % 3), (c // 3 + 1, c % 3)):
                if weight == 0:
                    continue
                group, at = divmod(plane * (bc + 1) + col, spare)
                src = group * LANES + nz * bf + at
                if plane < nz:
                    to_y[src, plane * bf + c] += weight
                else:
                    to_z[(plane - nz) * bf + c, src] += weight
    ey = along(gy * yc)
    return rows, along(gz * xc), to_y, to_z, ey, np.ascontiguousarray(ey.T)


def wrapped(index, size):
    return jnp.where(index >= size, index - size, index)


def kernel(gz, gy, nz, yc, xc, *refs):
    (scalar_hbm, vel_hbm, rows_hbm, ex_hbm, yy_hbm, zz_hbm, ey_hbm, eyt_hbm, out,
     scalar, vel, rows_m, ex_m, yy_m, zz_m, ey_m, eyt_m,
     xsend, wsend, own, nxt, other, blocks, pencil, speed_y,
     up_out, down_out, up_in, down_in,
     local_sem, own_s, own_r, nxt_s, nxt_r, oth_s, oth_r, blk_s, blk_r, z_s, z_r, ready) = refs
    h = lax.axis_index("gz")
    s = lax.axis_index("gy")
    rf = 3 * yc
    bc = gz * xc // gy
    bf = 3 * bc
    total = gz * nz
    nx = scalar.shape[2]
    ny = gy * rf
    behind, ahead = wrapped(s + gy - 1, gy), wrapped(s + 1, gy)

    loads = []
    for i, (src, dst) in enumerate((
        (vel_hbm, vel), (scalar_hbm, scalar), (rows_hbm, rows_m), (ex_hbm, ex_m),
        (yy_hbm, yy_m), (zz_hbm, zz_m), (ey_hbm, ey_m), (eyt_hbm, eyt_m),
    )):
        load = pltpu.make_async_copy(src, dst, local_sem.at[i])
        load.start()
        loads.append(load)

    barrier = pltpu.get_barrier_semaphore()

    def tell(semaphore, p, g):
        pl.semaphore_signal(
            semaphore, inc=1, device_id={"gz": p, "gy": g}, device_id_type=pl.DeviceIdType.MESH
        )

    def each(low, high, act):
        def one(i, _):
            act(i)
            return 0

        lax.fori_loop(low, high, one, 0)

    for step in range(1, gz):
        tell(barrier, wrapped(h + step, gz), s)
    for step in range(gz):
        tell(barrier, wrapped(h + step, gz), ahead)
    each(s + 1, gy, lambda g: tell(barrier, h, g))

    def remote(src, dst, send, recv, p, g):
        return pltpu.make_async_remote_copy(
            src_ref=src, dst_ref=dst, send_sem=send, recv_sem=recv,
            device_id={"gz": p, "gy": g}, device_id_type=pl.DeviceIdType.MESH,
        )

    loads[0].wait()
    fill = jnp.zeros((yc * xc, LANES - total), jnp.float32)

    def by_plane(c):
        wide = jnp.concatenate([vel[c].reshape(yc * xc, total), fill], axis=1)
        return jnp.transpose(wide)

    planes = by_plane(0)
    for p in range(gz):
        xsend[p] = planes[p * nz : (p + 1) * nz]
    planes = by_plane(1)
    for p in range(gz):
        wsend[p, :nz] = planes[p * nz : (p + 1) * nz]
    planes = by_plane(2)
    for p in range(gz):
        if p == 0:
            wsend[p, nz : nz + 1] = jnp.zeros((1, LANES), jnp.float32)
            wsend[p, nz + 1 :] = planes[: nz + 1]
        else:
            wsend[p, nz:] = planes[p * nz - 1 : (p + 1) * nz + 1]

    pl.semaphore_wait(barrier, 2 * gz - 1 + s)

    firsts, nexts, others = [], [], []
    for step in range(gz):
        p = wrapped(h + step, gz)
        if step:
            firsts.append(remote(xsend.at[p], own.at[h], own_s.at[step], own_r.at[h], p, s))
            others.append(remote(wsend.at[p], other.at[h], oth_s.at[step], oth_r.at[h], p, s))
        else:
            firsts.append(pltpu.make_async_copy(xsend.at[p], own.at[h], own_r.at[h]))
            others.append(pltpu.make_async_copy(wsend.at[p], other.at[h], oth_r.at[h]))
        nexts.append(remote(xsend.at[p], nxt.at[h], nxt_s.at[step], nxt_r.at[h], p, behind))
    for first, following in zip(firsts, nexts):
        first.start()
        following.start()
    for copy in others:
        copy.start()
    each(0, s, lambda g: tell(ready.at[s], h, g))

    lane = lax.broadcasted_iota(jnp.int32, (yc, LANES), 1)
    row = lax.broadcasted_iota(jnp.int32, (yc, LANES), 0)
    block = lane // xc

    def swap(value):
        for k in (1, 2, 4):
            row_bit, lane_bit = (row // k) % 2, (block // k) % 2
            value = jnp.where(
                row_bit == lane_bit,
                value,
                jnp.where(
                    row_bit == 0,
                    roll(roll(value, -k, 0), k * xc, 1),
                    roll(roll(value, k, 0), -k * xc, 1),
                ),
            )
        return value

    def spread(value):
        value = jnp.where(lane < xc, value, 0.0)
        for k in (1, 2, 4):
            value = jnp.where((row // k) % 2 == 1, roll(value, k * xc, 1), value)
        return jnp.sum(value, axis=0, keepdims=True)

    halves = [slice(i, i + yc) for i in range(0, gz, yc)]
    for i in range(gz):
        pltpu.make_async_copy(own.at[i], own.at[i], own_r.at[i]).wait()
        pltpu.make_async_copy(nxt.at[i], nxt.at[i], nxt_r.at[i]).wait()
    coarse = []
    for source, act in ((own, swap), (nxt, spread)):
        for z in range(nz):
            value = source[:, z, :]
            coarse.append(jnp.concatenate([act(value[half]) for half in halves], axis=1))
    coarse.append(jnp.zeros((8 - nz, gz * xc), jnp.float32))
    coarse = jnp.concatenate(coarse, axis=0)
    for load in loads[1:4]:
        load.wait()
    speed = exact_right(exact_left(rows_m[...], coarse), ex_m[...]) * NINTH
    field = scalar[...].reshape(nz * rf, nx)
    field = sweep_periodic(field, speed, 1)

    for i in range(gz):
        pltpu.make_async_copy(other.at[i], other.at[i], oth_r.at[i]).wait()
    kept = [[swap(other[:, k, :][half]) for half in halves] for k in range(2 * nz + 2)]
    wide = lax.broadcasted_iota(jnp.int32, (rf, LANES), 1)
    spare = LANES - nz * bf
    for g in range(gy):
        low = g * bf
        tile = None
        for z in range(nz):
            for t in range(low // LANES, (low + bf - 1) // LANES + 1):
                piece = field[z * rf : (z + 1) * rf, t * LANES : (t + 1) * LANES]
                begin = z * bf + max(0, t * LANES - low)
                moved = roll(piece, z * bf - low, 1)
                tile = moved if tile is None else jnp.where(wide >= begin, moved, tile)
        flat = jnp.zeros((yc, LANES), jnp.float32)
        for k in range(2 * nz + 2):
            at = k * (bc + 1)
            first = g * bc
            t, begin = divmod(first, LANES)
            flat = jnp.where(lane >= at, roll(kept[k][t], at - begin, 1), flat)
            if begin + bc == LANES:
                t = (t + 1) % len(halves)
                flat = jnp.where(lane >= at + bc, roll(kept[k][t], at + bc, 1), flat)
        flat = jnp.where(lane < (2 * nz + 2) * (bc + 1), flat, 0.0)
        extra = jnp.concatenate(
            [roll(flat, nz * bf - i * spare, 1) for i in range(rf // yc)], axis=0
        )
        blocks[g] = jnp.where(wide >= nz * bf, extra, tile)

    def block_copy(step):
        g = jnp.where(step <= s, s - step, step)
        if step == 0:
            return pltpu.make_async_copy(blocks.at[g], pencil.at[s], blk_r.at[s])
        return remote(blocks.at[g], pencil.at[s], blk_s.at[step], blk_r.at[s], h, g)

    sends = [block_copy(step) for step in range(gy)]
    sends[0].start()
    for step in range(1, gy):
        @pl.when(step > s)
        def _():
            pl.semaphore_wait(ready.at[step], 1)

        sends[step].start()

    for load in loads[4:]:
        load.wait()
    for i in range(gy):
        pltpu.make_async_copy(pencil.at[i], pencil.at[i], blk_r.at[i]).wait()
    nyc = gy * yc
    coarse = jnp.concatenate(
        [pencil[:, i : i + yc, :].reshape(nyc, LANES) for i in range(0, rf, yc)], axis=1
    )
    speed = exact_left(eyt_m[...], exact_right(coarse, yy_m[...])) * NINTH
    speed_y[EDGE : EDGE + ny] = speed
    speed_y[:EDGE] = speed[ny - EDGE :]
    speed_y[EDGE + ny :] = speed[:EDGE]
    speed_z = exact_right(exact_left(zz_m[...], coarse, ((1,), (1,))), ey_m[...]) * NINTH

    chunks = ny // LANES
    below, above = wrapped(h + gz - 1, gz), wrapped(h + 1, gz)
    whole = pencil[...].reshape(ny, LANES)
    around = jnp.concatenate([whole[ny - EDGE :], whole, whole[:EDGE]], axis=0)
    ups, downs = [], []
    for k in range(chunks):
        cols = slice(k * LANES, (k + 1) * LANES)
        rows = slice(k * LANES, (k + 1) * LANES + 2 * EDGE)
        swept = sweep_periodic(around[rows], speed_y[rows], 0)
        part = jnp.transpose(swept[EDGE : EDGE + LANES])[: nz * bf]
        moved = displacement(
            speed_z[bf : (nz + 1) * bf, cols], speed_z[: nz * bf, cols], speed_z[2 * bf :, cols]
        )
        w = weights(moved)

        def landing(target):
            result = None
            for m in range(-3, 4):
                z = target - m
                if 0 <= z < nz:
                    at = slice(z * bf, (z + 1) * bf)
                    term = part[at] * w[m][at]
                    result = term if result is None else result + term
            return result

        for i in range(3):
            up_out[k, i] = landing(nz + i)
            down_out[k, i] = landing(i - 3)
        up = remote(up_out.at[k], up_in.at[k], z_s.at[0, k], z_r.at[0, k], above, s)
        down = remote(down_out.at[k], down_in.at[k], z_s.at[1, k], z_r.at[1, k], below, s)
        ups.append(up)
        downs.append(down)

        @pl.when(h < gz - 1)
        def _():
            up.start()

        @pl.when(h > 0)
        def _():
            down.start()

        for i in range(nz):
            out[i, :, cols] = landing(i)

    @pl.when(h > 0)
    def _():
        for k in range(chunks):
            cols = slice(k * LANES, (k + 1) * LANES)
            ups[k].wait_recv()
            for i in range(3):
                out[i, :, cols] = out[i, :, cols] + up_in[k, i]
        for copy in downs:
            copy.wait_send()

    @pl.when(h < gz - 1)
    def _():
        for k in range(chunks):
            cols = slice(k * LANES, (k + 1) * LANES)
            downs[k].wait_recv()
            for i in range(nz - 3, nz):
                out[i, :, cols] = out[i, :, cols] + down_in[k, i - nz + 3]
        for copy in ups:
            copy.wait_send()

    for copy in sends[1:] + firsts[1:] + nexts + others[1:]:
        copy.wait_send()


def local(scalar, velocity):
    gz, gy = lax.axis_size("gz"), lax.axis_size("gy")
    nz, rf, nx = scalar.shape
    yc, xc = velocity.shape[2:]
    bc = gz * xc // gy
    bf = 3 * bc
    ny = gy * rf
    mats = [jnp.asarray(m, jnp.bfloat16) for m in constants(nz, gz, gy, yc, xc)]
    turned = jnp.transpose(velocity, (0, 2, 3, 1))
    f32 = jnp.float32
    dma = pltpu.SemaphoreType.DMA
    anywhere = pl.BlockSpec(memory_space=pl.ANY)
    vmem = pl.BlockSpec(memory_space=pltpu.VMEM)
    scratch = [pltpu.VMEM(scalar.shape, f32), pltpu.VMEM(turned.shape, f32)]
    scratch += [pltpu.VMEM(m.shape, jnp.bfloat16) for m in mats]
    scratch += [
        pltpu.VMEM((gz, nz, LANES), f32),
        pltpu.VMEM((gz, 2 * nz + 2, LANES), f32),
        pltpu.VMEM((gz, nz, LANES), f32),
        pltpu.VMEM((gz, nz, LANES), f32),
        pltpu.VMEM((gz, 2 * nz + 2, LANES), f32),
        pltpu.VMEM((gy, rf, LANES), f32),
        pltpu.VMEM((gy, rf, LANES), f32),
        pltpu.VMEM((ny + 2 * EDGE, LANES), f32),
    ]
    scratch += [pltpu.VMEM((ny // LANES, 3, bf, LANES), f32)] * 4
    scratch += [dma((n,)) for n in (2 + len(mats), gz, gz, gz, gz, gz, gz, gy, gy)]
    scratch += [dma((2, ny // LANES))] * 2
    scratch += [pltpu.SemaphoreType.REGULAR((gy,))]
    return pl.pallas_call(
        functools.partial(kernel, gz, gy, nz, yc, xc),
        out_shape=pltpu.VMEM((nz, bf, ny), f32),
        in_specs=[anywhere] * (2 + len(mats)),
        out_specs=vmem,
        scratch_shapes=scratch,
        compiler_params=pltpu.CompilerParams(has_side_effects=True, collective_id=0),
    )(scalar, turned, *mats)


def solution(mesh):
    in_specs = (P("gz", "gy", None), P(None, None, "gy", "gz"))
    out_specs = P("gz", "gy", None)
    return jax.shard_map(local, mesh=mesh, in_specs=in_specs, out_specs=out_specs, check_vma=False)
```

```python
import functools

import jax
import jax.numpy as jnp
import numpy as np
from jax import lax
from jax.experimental import pallas as pl
from jax.experimental.pallas import tpu as pltpu
from jax.sharding import PartitionSpec as P

LANES = 128
INNER = [1.0, 0.0, -5.0 / 4.0, -35.0 / 12.0, 21.0 / 4.0, -25.0 / 12.0]
MIDDLE = [-4.0, 75.0 / 4.0, -245.0 / 8.0, 545.0 / 24.0, -63.0 / 8.0, 25.0 / 24.0]
OUTER = [18.0, -153.0 / 4.0, 255.0 / 8.0, -313.0 / 24.0, 21.0 / 8.0, -5.0 / 24.0]


def shifted(factors, base, slope):
    total = np.polynomial.Polynomial([0.0])
    for factor in reversed(factors):
        total = total * np.polynomial.Polynomial([base, slope]) + factor
    coefs = np.zeros(6)
    coefs[: len(total.coef)] = total.coef
    return [0.0 if abs(c) < 1e-10 else float(c) for c in coefs]


AHEAD = {1: shifted(INNER, 1.0, -1.0), 2: shifted(MIDDLE, 2.0, -1.0), 3: shifted(OUTER, 3.0, -1.0)}
BEHIND = {1: shifted(MIDDLE, 1.0, 1.0), 2: shifted(OUTER, 2.0, 1.0)}


def horner(factors, value):
    lowest = 0
    while factors[lowest] == 0.0:
        lowest += 1
    result = jnp.full_like(value, factors[-1])
    for factor in reversed(factors[lowest:-1]):
        result = result * value
        if factor != 0.0:
            result = result + factor
    for _ in range(lowest):
        result = result * value
    return result


def weights(moved):
    size = jnp.abs(moved)
    positive = moved >= 0.0
    result = {0: horner(INNER, size)}
    for m in (1, 2, 3):
        near = horner(AHEAD[m], size)
        far = horner(BEHIND[m], size) if m in BEHIND else jnp.zeros_like(size)
        result[m] = jnp.where(positive, near, far)
        result[-m] = jnp.where(positive, far, near)
    return result


def displacement(speed, before, after):
    return speed + 0.5 * speed * jnp.where(speed >= 0.0, after - speed, speed - before)


def roll(value, shift, axis):
    return pltpu.roll(value, shift % value.shape[axis], axis)


def sweep_periodic(field, speed, axis):
    moved = displacement(speed, roll(speed, 1, axis), roll(speed, -1, axis))
    w = weights(moved)
    result = field * w[0]
    for m in (-3, -2, -1, 1, 2, 3):
        result = result + roll(field * w[m], m, axis)
    return result


def split(value):
    high = value.astype(jnp.bfloat16)
    return high, (value - high.astype(jnp.float32)).astype(jnp.bfloat16)


def dot(a, b, dims=((1,), (0,))):
    return lax.dot_general(a, b, (dims, ((), ())), preferred_element_type=jnp.float32)


def exact_left(a, value, dims=((1,), (0,))):
    high, low = split(value)
    return dot(a, high, dims) + dot(a, low, dims)


def exact_right(value, b):
    high, low = split(value)
    return dot(high, b) + dot(low, b)


EDGE = 8
REACH = 4
SPAN = 8


def touched(chunk, yc):
    first, end = chunk * LANES - REACH, (chunk + 1) * LANES + REACH
    low = min((first // 3) // yc, (chunk * LANES - EDGE) // (3 * yc))
    high = max(((end - 1) // 3 + 1) // yc, ((chunk + 1) * LANES + EDGE - 1) // (3 * yc))
    assert high - low < SPAN
    return low, high


NINTH = 1.0 / 9.0


def along(count):
    out = np.zeros((count, 3 * count), np.float32)
    for c in range(count):
        for k in range(3):
            out[c, 3 * c + k] += 3 - k
            out[(c + 1) % count, 3 * c + k] += k
    return out


def constants(nz, gz, gy, yc, xc):
    bc = gz * xc // gy
    bf = 3 * bc
    rf = 3 * yc
    spare = LANES - nz * bf
    rows = np.zeros((nz * rf, nz * yc + 8), np.float32)
    for z in range(nz):
        for r in range(rf):
            y, k = divmod(r, 3)
            rows[z * rf + r, z * yc + y] += 3 - k
            rows[z * rf + r, z * yc + y + 1 if y < yc - 1 else nz * yc + z] += k
    groups = rf // yc
    to_y = np.zeros((groups * LANES, LANES), np.float32)
    to_z = np.zeros(((nz + 2) * bf, groups * LANES), np.float32)
    for plane in range(2 * nz + 2):
        for c in range(bf):
            for col, weight in ((c // 3, 3 - c % 3), (c // 3 + 1, c % 3)):
                if weight == 0:
                    continue
                group, at = divmod(plane * (bc + 1) + col, spare)
                src = group * LANES + nz * bf + at
                if plane < nz:
                    to_y[src, plane * bf + c] += weight
                else:
                    to_z[(plane - nz) * bf + c, src] += weight
    chunks = gy * rf // LANES
    down = np.zeros((chunks, LANES + 2 * EDGE, SPAN * yc), np.float32)
    across = np.zeros((chunks, SPAN * yc, LANES), np.float32)
    for chunk in range(chunks):
        base = yc * touched(chunk, yc)[0]
        for r in range(-REACH, LANES + REACH):
            c, k = divmod(chunk * LANES + r, 3)
            for at, weight in ((c - base, 3 - k), (c + 1 - base, k)):
                if weight:
                    down[chunk, EDGE + r, at] += weight
                    if 0 <= r < LANES:
                        across[chunk, at, r] += weight
    return rows, along(gz * xc), to_y, to_z, across, down


def wrapped(index, size):
    return jnp.where(index >= size, index - size, index)


def kernel(gz, gy, nz, yc, xc, *refs):
    (scalar_hbm, vel_hbm, rows_hbm, ex_hbm, yy_hbm, zz_hbm, ey_hbm, eyt_hbm, out,
     scalar, vel, rows_m, ex_m, yy_m, zz_m, ey_m, eyt_m,
     xsend, wsend, own, nxt, other, kept, blocks, pencil,
     up_out, down_out, up_in, down_in,
     local_sem, own_s, own_r, nxt_s, nxt_r, oth_s, oth_r, blk_s, blk_r, z_s, z_r, ready) = refs
    h = lax.axis_index("gz")
    s = lax.axis_index("gy")
    rf = 3 * yc
    bc = gz * xc // gy
    bf = 3 * bc
    total = gz * nz
    nx = scalar.shape[2]
    ny = gy * rf
    behind, ahead = wrapped(s + gy - 1, gy), wrapped(s + 1, gy)

    loads = []
    for i, (src, dst) in enumerate((
        (vel_hbm, vel), (scalar_hbm, scalar), (rows_hbm, rows_m), (ex_hbm, ex_m),
        (yy_hbm, yy_m), (zz_hbm, zz_m), (ey_hbm, ey_m), (eyt_hbm, eyt_m),
    )):
        load = pltpu.make_async_copy(src, dst, local_sem.at[i])
        load.start()
        loads.append(load)

    barrier = pltpu.get_barrier_semaphore()

    def tell(semaphore, p, g):
        pl.semaphore_signal(
            semaphore, inc=1, device_id={"gz": p, "gy": g}, device_id_type=pl.DeviceIdType.MESH
        )

    def each(low, high, act):
        def one(i, _):
            act(i)
            return 0

        lax.fori_loop(low, high, one, 0)

    for step in range(1, gz):
        tell(barrier, wrapped(h + step, gz), s)
    for step in range(gz):
        tell(barrier, wrapped(h + step, gz), ahead)
    each(s + 1, gy, lambda g: tell(barrier, h, g))

    def remote(src, dst, send, recv, p, g):
        return pltpu.make_async_remote_copy(
            src_ref=src, dst_ref=dst, send_sem=send, recv_sem=recv,
            device_id={"gz": p, "gy": g}, device_id_type=pl.DeviceIdType.MESH,
        )

    loads[0].wait()
    fill = jnp.zeros((yc * xc, LANES - total), jnp.float32)

    def by_plane(c):
        wide = jnp.concatenate([vel[c].reshape(yc * xc, total), fill], axis=1)
        return jnp.transpose(wide)

    planes = by_plane(0)
    for p in range(gz):
        xsend[p] = planes[p * nz : (p + 1) * nz]
    planes = by_plane(1)
    for p in range(gz):
        wsend[p, :nz] = planes[p * nz : (p + 1) * nz]
    planes = by_plane(2)
    for p in range(gz):
        if p == 0:
            wsend[p, nz : nz + 1] = jnp.zeros((1, LANES), jnp.float32)
            wsend[p, nz + 1 :] = planes[: nz + 1]
        else:
            wsend[p, nz:] = planes[p * nz - 1 : (p + 1) * nz + 1]

    pl.semaphore_wait(barrier, 2 * gz - 1 + s)

    firsts, nexts, others = [], [], []
    for step in range(gz):
        p = wrapped(h + step, gz)
        if step:
            firsts.append(remote(xsend.at[p], own.at[h], own_s.at[step], own_r.at[h], p, s))
            others.append(remote(wsend.at[p], other.at[h], oth_s.at[step], oth_r.at[h], p, s))
        else:
            firsts.append(pltpu.make_async_copy(xsend.at[p], own.at[h], own_r.at[h]))
            others.append(pltpu.make_async_copy(wsend.at[p], other.at[h], oth_r.at[h]))
        nexts.append(remote(xsend.at[p], nxt.at[h], nxt_s.at[step], nxt_r.at[h], p, behind))
    for first, following in zip(firsts, nexts):
        first.start()
        following.start()
    for copy in others:
        copy.start()
    each(0, s, lambda g: tell(ready.at[s], h, g))

    lane = lax.broadcasted_iota(jnp.int32, (yc, LANES), 1)
    row = lax.broadcasted_iota(jnp.int32, (yc, LANES), 0)
    block = lane // xc

    def swap(value):
        for k in (1, 2, 4):
            row_bit, lane_bit = (row // k) % 2, (block // k) % 2
            value = jnp.where(
                row_bit == lane_bit,
                value,
                jnp.where(
                    row_bit == 0,
                    roll(roll(value, -k, 0), k * xc, 1),
                    roll(roll(value, k, 0), -k * xc, 1),
                ),
            )
        return value

    def spread(value):
        value = jnp.where(lane < xc, value, 0.0)
        for k in (1, 2, 4):
            value = jnp.where((row // k) % 2 == 1, roll(value, k * xc, 1), value)
        return jnp.sum(value, axis=0, keepdims=True)

    halves = [slice(i, i + yc) for i in range(0, gz, yc)]
    for i in range(gz):
        pltpu.make_async_copy(own.at[i], own.at[i], own_r.at[i]).wait()
        pltpu.make_async_copy(nxt.at[i], nxt.at[i], nxt_r.at[i]).wait()
    coarse = []
    for source, act in ((own, swap), (nxt, spread)):
        for z in range(nz):
            value = source[:, z, :]
            coarse.append(jnp.concatenate([act(value[half]) for half in halves], axis=1))
    coarse.append(jnp.zeros((8 - nz, gz * xc), jnp.float32))
    coarse = jnp.concatenate(coarse, axis=0)
    for load in loads[1:4]:
        load.wait()
    speed = exact_right(exact_left(rows_m[...], coarse), ex_m[...]) * NINTH
    field = scalar[...].reshape(nz * rf, nx)
    field = sweep_periodic(field, speed, 1)
    for z in range(nz):
        scalar[z] = field[z * rf : (z + 1) * rf]

    for i in range(gz):
        pltpu.make_async_copy(other.at[i], other.at[i], oth_r.at[i]).wait()
    for k in range(2 * nz + 2):
        parts = [swap(other[:, k, :][half]) for half in halves]
        for t, part in enumerate(parts + parts[:1]):
            kept[k, :, t * LANES : (t + 1) * LANES] = part
    wide = lax.broadcasted_iota(jnp.int32, (rf, LANES), 1)
    spare = LANES - nz * bf
    last = nx // LANES - 1

    def build(step):
        g = jnp.where(step <= s, s - step, step)
        low = g * bf
        t = lax.div(low, LANES)
        here = pl.ds(pl.multiple_of(t * LANES, LANES), LANES)
        there = pl.ds(pl.multiple_of(jnp.minimum(t + 1, last) * LANES, LANES), LANES)
        tile = None
        for z in range(nz):
            piece = jnp.where(
                wide < low + bf - (t + 1) * LANES, scalar[z, :, there], scalar[z, :, here]
            )
            piece = pltpu.roll(piece, lax.rem(z * bf + nx - low, LANES), 1)
            tile = piece if tile is None else jnp.where(wide >= z * bf, piece, tile)
        first = g * bc
        t = lax.div(first, LANES)
        here = pl.ds(pl.multiple_of(t * LANES, LANES), LANES)
        there = pl.ds(pl.multiple_of((t + 1) * LANES, LANES), LANES)
        flat = None
        for k in range(2 * nz + 2):
            at = k * (bc + 1)
            piece = jnp.where(
                lane < first + bc + 1 - (t + 1) * LANES, kept[k, :, there], kept[k, :, here]
            )
            piece = pltpu.roll(piece, lax.rem(at + nx - first, LANES), 1)
            flat = piece if flat is None else jnp.where(lane >= at, piece, flat)
        flat = jnp.where(lane < (2 * nz + 2) * (bc + 1), flat, 0.0)
        extra = jnp.concatenate(
            [roll(flat, nz * bf - i * spare, 1) for i in range(rf // yc)], axis=0
        )
        blocks[step] = jnp.where(wide >= nz * bf, extra, tile)

    def block_copy(step):
        g = jnp.where(step <= s, s - step, step)
        return remote(blocks.at[step], pencil.at[s], blk_s.at[step], blk_r.at[s], h, g)

    def send(step):
        @pl.when(step > s)
        def _():
            pl.semaphore_wait(ready.at[step], 1)

        block_copy(step).start()

    def pair(i):
        build(2 * i + 1)
        build(2 * i + 2)
        send(2 * i + 1)
        send(2 * i + 2)

    each(0, gy // 2 - 1, pair)
    build(gy - 1)
    send(gy - 1)
    build(0)
    pltpu.make_async_copy(blocks.at[0], pencil.at[s], blk_r.at[s]).start()

    for load in loads[4:]:
        load.wait()
    chunks = ny // LANES
    order = list(range(1, chunks)) + [0]
    here = set()
    below, above = wrapped(h + gz - 1, gz), wrapped(h + 1, gz)
    ups, downs = {}, {}
    for k in order:
        cols = slice(k * LANES, (k + 1) * LANES)
        low, high = touched(k, yc)
        gs = [g % gy for g in range(low, high + 1)]
        for g in gs:
            if g not in here:
                here.add(g)
                pltpu.make_async_copy(pencil.at[g], pencil.at[g], blk_r.at[g]).wait()
        got = jnp.concatenate([pencil[g] for g in gs], axis=0)
        coarse = [
            jnp.concatenate([pencil[g, i : i + yc, :] for g in gs], axis=0)
            for i in range(0, rf, yc)
        ]
        coarse = jnp.concatenate(coarse, axis=1)
        if len(gs) < SPAN:
            coarse = jnp.concatenate(
                [coarse, jnp.zeros(((SPAN - len(gs)) * yc, coarse.shape[1]), jnp.float32)], axis=0
            )
        for_y = exact_right(coarse, yy_m[...])
        for_z = exact_left(zz_m[...], coarse, ((1,), (1,)))
        speed_y = exact_left(eyt_m[k], for_y) * NINTH
        speed_z = exact_right(for_z, ey_m[k]) * NINTH
        start = k * LANES - EDGE - low * rf
        swept = sweep_periodic(got[start : start + LANES + 2 * EDGE], speed_y, 0)
        part = jnp.transpose(swept[EDGE : EDGE + LANES])[: nz * bf]
        moved = displacement(
            speed_z[bf : (nz + 1) * bf], speed_z[: nz * bf], speed_z[2 * bf :]
        )
        w = weights(moved)

        def landing(target):
            result = None
            for m in range(-3, 4):
                z = target - m
                if 0 <= z < nz:
                    at = slice(z * bf, (z + 1) * bf)
                    term = part[at] * w[m][at]
                    result = term if result is None else result + term
            return result

        for i in range(3):
            up_out[k, i] = landing(nz + i)
            down_out[k, i] = landing(i - 3)
        up = remote(up_out.at[k], up_in.at[k], z_s.at[0, k], z_r.at[0, k], above, s)
        down = remote(down_out.at[k], down_in.at[k], z_s.at[1, k], z_r.at[1, k], below, s)
        ups[k], downs[k] = up, down

        @pl.when(h < gz - 1)
        def _():
            up.start()

        @pl.when(h > 0)
        def _():
            down.start()

        for i in range(nz):
            out[i, :, cols] = landing(i)

    @pl.when(h > 0)
    def _():
        for k in order:
            cols = slice(k * LANES, (k + 1) * LANES)
            ups[k].wait_recv()
            for i in range(3):
                out[i, :, cols] = out[i, :, cols] + up_in[k, i]
        for copy in downs.values():
            copy.wait_send()

    @pl.when(h < gz - 1)
    def _():
        for k in order:
            cols = slice(k * LANES, (k + 1) * LANES)
            downs[k].wait_recv()
            for i in range(nz - 3, nz):
                out[i, :, cols] = out[i, :, cols] + down_in[k, i - nz + 3]
        for copy in ups.values():
            copy.wait_send()

    for copy in firsts[1:] + nexts + others[1:]:
        copy.wait_send()
    each(1, gy, lambda step: block_copy(step).wait_send())


def local(scalar, velocity):
    gz, gy = lax.axis_size("gz"), lax.axis_size("gy")
    nz, rf, nx = scalar.shape
    yc, xc = velocity.shape[2:]
    bc = gz * xc // gy
    bf = 3 * bc
    ny = gy * rf
    mats = [jnp.asarray(m, jnp.bfloat16) for m in constants(nz, gz, gy, yc, xc)]
    turned = jnp.transpose(velocity, (0, 2, 3, 1))
    f32 = jnp.float32
    dma = pltpu.SemaphoreType.DMA
    anywhere = pl.BlockSpec(memory_space=pl.ANY)
    vmem = pl.BlockSpec(memory_space=pltpu.VMEM)
    scratch = [pltpu.VMEM(scalar.shape, f32), pltpu.VMEM(turned.shape, f32)]
    scratch += [pltpu.VMEM(m.shape, jnp.bfloat16) for m in mats]
    scratch += [
        pltpu.VMEM((gz, nz, LANES), f32),
        pltpu.VMEM((gz, 2 * nz + 2, LANES), f32),
        pltpu.VMEM((gz, nz, LANES), f32),
        pltpu.VMEM((gz, nz, LANES), f32),
        pltpu.VMEM((gz, 2 * nz + 2, LANES), f32),
        pltpu.VMEM((2 * nz + 2, yc, gz * xc + LANES), f32),
        pltpu.VMEM((gy, rf, LANES), f32),
        pltpu.VMEM((gy, rf, LANES), f32),
    ]
    scratch += [pltpu.VMEM((ny // LANES, 3, bf, LANES), f32)] * 4
    scratch += [dma((n,)) for n in (2 + len(mats), gz, gz, gz, gz, gz, gz, gy, gy)]
    scratch += [dma((2, ny // LANES))] * 2
    scratch += [pltpu.SemaphoreType.REGULAR((gy,))]
    return pl.pallas_call(
        functools.partial(kernel, gz, gy, nz, yc, xc),
        out_shape=pltpu.VMEM((nz, bf, ny), f32),
        in_specs=[anywhere] * (2 + len(mats)),
        out_specs=vmem,
        scratch_shapes=scratch,
        compiler_params=pltpu.CompilerParams(has_side_effects=True, collective_id=0),
    )(scalar, turned, *mats)


def solution(mesh):
    in_specs = (P("gz", "gy", None), P(None, None, "gy", "gz"))
    out_specs = P("gz", "gy", None)
    return jax.shard_map(local, mesh=mesh, in_specs=in_specs, out_specs=out_specs, check_vma=False)
```

```python
import functools

import jax
import jax.numpy as jnp
import numpy as np
from jax import lax
from jax.experimental import pallas as pl
from jax.experimental.pallas import tpu as pltpu
from jax.sharding import PartitionSpec as P

LANES = 128
INNER = [1.0, 0.0, -5.0 / 4.0, -35.0 / 12.0, 21.0 / 4.0, -25.0 / 12.0]
MIDDLE = [-4.0, 75.0 / 4.0, -245.0 / 8.0, 545.0 / 24.0, -63.0 / 8.0, 25.0 / 24.0]
OUTER = [18.0, -153.0 / 4.0, 255.0 / 8.0, -313.0 / 24.0, 21.0 / 8.0, -5.0 / 24.0]


def shifted(factors, base, slope):
    total = np.polynomial.Polynomial([0.0])
    for factor in reversed(factors):
        total = total * np.polynomial.Polynomial([base, slope]) + factor
    coefs = np.zeros(6)
    coefs[: len(total.coef)] = total.coef
    return [0.0 if abs(c) < 1e-10 else float(c) for c in coefs]


AHEAD = {1: shifted(INNER, 1.0, -1.0), 2: shifted(MIDDLE, 2.0, -1.0), 3: shifted(OUTER, 3.0, -1.0)}
BEHIND = {1: shifted(MIDDLE, 1.0, 1.0), 2: shifted(OUTER, 2.0, 1.0)}


def horner(factors, value):
    lowest = 0
    while factors[lowest] == 0.0:
        lowest += 1
    result = jnp.full_like(value, factors[-1])
    for factor in reversed(factors[lowest:-1]):
        result = result * value
        if factor != 0.0:
            result = result + factor
    for _ in range(lowest):
        result = result * value
    return result


def weights(moved):
    size = jnp.abs(moved)
    positive = moved >= 0.0
    result = {0: horner(INNER, size)}
    for m in (1, 2, 3):
        near = horner(AHEAD[m], size)
        far = horner(BEHIND[m], size) if m in BEHIND else jnp.zeros_like(size)
        result[m] = jnp.where(positive, near, far)
        result[-m] = jnp.where(positive, far, near)
    return result


def displacement(speed, before, after):
    return speed + 0.5 * speed * jnp.where(speed >= 0.0, after - speed, speed - before)


def roll(value, shift, axis):
    return pltpu.roll(value, shift % value.shape[axis], axis)


def sweep_periodic(field, speed, axis):
    moved = displacement(speed, roll(speed, 1, axis), roll(speed, -1, axis))
    w = weights(moved)
    result = field * w[0]
    for m in (-3, -2, -1, 1, 2, 3):
        result = result + roll(field * w[m], m, axis)
    return result


def split(value):
    high = value.astype(jnp.bfloat16)
    return high, (value - high.astype(jnp.float32)).astype(jnp.bfloat16)


def dot(a, b, dims=((1,), (0,))):
    return lax.dot_general(a, b, (dims, ((), ())), preferred_element_type=jnp.float32)


def exact_left(a, value, dims=((1,), (0,))):
    high, low = split(value)
    return dot(a, high, dims) + dot(a, low, dims)


def exact_right(value, b):
    high, low = split(value)
    return dot(high, b) + dot(low, b)


EDGE = 8
REACH = 4
SPAN = 24
TURN = 4
WIDTHS = (1, 1, 1, 3)


def windows(chunks):
    out, at = [], 1
    while at <= chunks:
        width = min(WIDTHS[len(out) % len(WIDTHS)], chunks + 1 - at)
        out.append((at, width))
        at += width
    return out


def touched(chunk, width, yc):
    first, end = chunk * LANES, (chunk + width) * LANES
    low = min(((first - REACH) // 3) // yc, (first - EDGE) // (3 * yc))
    high = max(((end + REACH - 1) // 3 + 1) // yc, (end + EDGE - 1) // (3 * yc))
    assert high - low < SPAN
    return low, high


NINTH = 1.0 / 9.0


def along(count):
    out = np.zeros((count, 3 * count), np.float32)
    for c in range(count):
        for k in range(3):
            out[c, 3 * c + k] += 3 - k
            out[(c + 1) % count, 3 * c + k] += k
    return out


def constants(nz, gz, gy, yc, xc):
    bc = gz * xc // gy
    bf = 3 * bc
    rf = 3 * yc
    spare = LANES - nz * bf
    rows = np.zeros((nz * rf, nz * yc + 8), np.float32)
    for z in range(nz):
        for r in range(rf):
            y, k = divmod(r, 3)
            rows[z * rf + r, z * yc + y] += 3 - k
            rows[z * rf + r, z * yc + y + 1 if y < yc - 1 else nz * yc + z] += k
    groups = rf // yc
    to_y = np.zeros((groups * LANES, LANES), np.float32)
    to_z = np.zeros(((nz + 2) * bf, groups * LANES), np.float32)
    for plane in range(2 * nz + 2):
        for c in range(bf):
            for col, weight in ((c // 3, 3 - c % 3), (c // 3 + 1, c % 3)):
                if weight == 0:
                    continue
                group, at = divmod(plane * (bc + 1) + col, spare)
                src = group * LANES + nz * bf + at
                if plane < nz:
                    to_y[src, plane * bf + c] += weight
                else:
                    to_z[(plane - nz) * bf + c, src] += weight
    parts = windows(gy * rf // LANES)
    most = LANES * max(width for _, width in parts)
    down = np.zeros((len(parts), most + 2 * EDGE, SPAN * yc), np.float32)
    across = np.zeros((len(parts), SPAN * yc, most), np.float32)
    for i, (chunk, width) in enumerate(parts):
        base = yc * touched(chunk, width, yc)[0]
        for r in range(-REACH, width * LANES + REACH):
            c, k = divmod(chunk * LANES + r, 3)
            for at, weight in ((c - base, 3 - k), (c + 1 - base, k)):
                if weight:
                    down[i, EDGE + r, at] += weight
                    if 0 <= r < width * LANES:
                        across[i, at, r] += weight
    return rows, along(gz * xc), to_y, to_z, across, down


def wrapped(index, size):
    return jnp.where(index >= size, index - size, index)


def kernel(gz, gy, nz, yc, xc, *refs):
    (scalar_hbm, vel_hbm, rows_hbm, ex_hbm, yy_hbm, zz_hbm, ey_hbm, eyt_hbm, out,
     scalar, vel, rows_m, ex_m, yy_m, zz_m, ey_m, eyt_m,
     xsend, nsend, wsend, own, nxt, other, kept, blocks, pencil,
     up_out, down_out, up_in, down_in,
     local_sem, own_s, own_r, nxt_s, nxt_r, oth_s, oth_r, blk_s, blk_r, z_s, z_r, ready) = refs
    h = lax.axis_index("gz")
    s = lax.axis_index("gy")
    rf = 3 * yc
    bc = gz * xc // gy
    bf = 3 * bc
    total = gz * nz
    nx = scalar.shape[2]
    ny = gy * rf
    behind, ahead = wrapped(s + gy - 1, gy), wrapped(s + 1, gy)

    loads = []
    for i, (src, dst) in enumerate((
        (vel_hbm, vel), (scalar_hbm, scalar), (rows_hbm, rows_m), (ex_hbm, ex_m),
        (yy_hbm, yy_m), (zz_hbm, zz_m), (ey_hbm, ey_m), (eyt_hbm, eyt_m),
    )):
        load = pltpu.make_async_copy(src, dst, local_sem.at[i])
        load.start()
        loads.append(load)

    barrier = pltpu.get_barrier_semaphore()

    def tell(semaphore, p, g):
        pl.semaphore_signal(
            semaphore, inc=1, device_id={"gz": p, "gy": g}, device_id_type=pl.DeviceIdType.MESH
        )

    def each(low, high, act):
        def one(i, _):
            act(i)
            return 0

        lax.fori_loop(low, high, one, 0)

    for step in range(1, gz):
        tell(barrier, wrapped(h + step, gz), s)
    for step in range(gz):
        tell(barrier, wrapped(h + step, gz), ahead)
    each(s + 1, gy, lambda g: tell(barrier, h, g))

    def remote(src, dst, send, recv, p, g):
        return pltpu.make_async_remote_copy(
            src_ref=src, dst_ref=dst, send_sem=send, recv_sem=recv,
            device_id={"gz": p, "gy": g}, device_id_type=pl.DeviceIdType.MESH,
        )

    loads[0].wait()
    fill = jnp.zeros((yc * xc, LANES - total), jnp.float32)

    def by_plane(c):
        wide = jnp.concatenate([vel[c].reshape(yc * xc, total), fill], axis=1)
        return jnp.transpose(wide)

    planes = by_plane(0)
    for p in range(gz):
        xsend[p] = planes[p * nz : (p + 1) * nz]
    tall = lax.broadcasted_iota(jnp.int32, (LANES, LANES), 0)
    bottom = jnp.where(lax.broadcasted_iota(jnp.int32, (LANES, LANES), 1) < xc, planes, 0.0)
    shifts = [roll(bottom, i * xc, 1) if i else bottom for i in range(nz)]
    bottom = shifts[0]
    for i in range(1, nz):
        bottom = jnp.where(tall % nz == i, shifts[i], bottom)
    for p in range(gz):
        nsend[p] = jnp.sum(bottom[p * nz : (p + 1) * nz], axis=0, keepdims=True)
    planes = by_plane(1)
    for p in range(gz):
        wsend[p, :nz] = planes[p * nz : (p + 1) * nz]
    planes = by_plane(2)
    for p in range(gz):
        if p == 0:
            wsend[p, nz : nz + 1] = jnp.zeros((1, LANES), jnp.float32)
            wsend[p, nz + 1 :] = planes[: nz + 1]
        else:
            wsend[p, nz:] = planes[p * nz - 1 : (p + 1) * nz + 1]

    pl.semaphore_wait(barrier, 2 * gz - 1 + s)

    firsts, nexts, others = [], [], []
    for step in range(gz):
        p = wrapped(h + step, gz)
        if step:
            firsts.append(remote(xsend.at[p], own.at[h], own_s.at[step], own_r.at[h], p, s))
            others.append(remote(wsend.at[p], other.at[h], oth_s.at[step], oth_r.at[h], p, s))
        else:
            firsts.append(pltpu.make_async_copy(xsend.at[p], own.at[h], own_r.at[h]))
            others.append(pltpu.make_async_copy(wsend.at[p], other.at[h], oth_r.at[h]))
        nexts.append(remote(nsend.at[p], nxt.at[h], nxt_s.at[step], nxt_r.at[h], p, behind))
    for copy in firsts + nexts + others:
        copy.start()
    each(0, s, lambda g: tell(ready.at[s], h, g))

    lane = lax.broadcasted_iota(jnp.int32, (yc, LANES), 1)
    row = lax.broadcasted_iota(jnp.int32, (yc, LANES), 0)
    block = lane // xc

    def swap(value):
        for k in (1, 2, 4):
            row_bit, lane_bit = (row // k) % 2, (block // k) % 2
            value = jnp.where(
                row_bit == lane_bit,
                value,
                jnp.where(
                    row_bit == 0,
                    roll(roll(value, -k, 0), k * xc, 1),
                    roll(roll(value, k, 0), -k * xc, 1),
                ),
            )
        return value

    halves = [slice(i, i + yc) for i in range(0, gz, yc)]
    for i in range(gz):
        pltpu.make_async_copy(own.at[i], own.at[i], own_r.at[i]).wait()
        pltpu.make_async_copy(nxt.at[i], nxt.at[i], nxt_r.at[i]).wait()
    coarse = []
    for value in [own[:, z, :] for z in range(nz)] + [nxt[:, 0, :]]:
        coarse.append(jnp.concatenate([swap(value[half]) for half in halves], axis=1))
    coarse = jnp.concatenate(coarse, axis=0)
    for load in loads[1:4]:
        load.wait()
    speed = exact_right(exact_left(rows_m[...], coarse), ex_m[...]) * NINTH
    field = scalar[...].reshape(nz * rf, nx)
    field = sweep_periodic(field, speed, 1)
    for z in range(nz):
        scalar[z] = field[z * rf : (z + 1) * rf]

    for i in range(gz):
        pltpu.make_async_copy(other.at[i], other.at[i], oth_r.at[i]).wait()
    for k in range(2 * nz + 2):
        parts = [swap(other[:, k, :][half]) for half in halves]
        for t, part in enumerate(parts + parts[:1]):
            kept[k, :, t * LANES : (t + 1) * LANES] = part
    wide = lax.broadcasted_iota(jnp.int32, (rf, LANES), 1)
    spare = LANES - nz * bf
    last = nx // LANES - 1

    def target(step):
        near = jnp.where(step <= s, s - step, step)
        return jnp.where(s >= 3 * gy // 4, wrapped(s + step, gy), near)

    def build(step):
        g = target(step)
        low = g * bf
        t = lax.div(low, LANES)
        here = pl.ds(pl.multiple_of(t * LANES, LANES), LANES)
        there = pl.ds(pl.multiple_of(jnp.minimum(t + 1, last) * LANES, LANES), LANES)
        tile = None
        for z in range(nz):
            piece = jnp.where(
                wide < low + bf - (t + 1) * LANES, scalar[z, :, there], scalar[z, :, here]
            )
            piece = pltpu.roll(piece, lax.rem(z * bf + nx - low, LANES), 1)
            tile = piece if tile is None else jnp.where(wide >= z * bf, piece, tile)
        first = g * bc
        t = lax.div(first, LANES)
        here = pl.ds(pl.multiple_of(t * LANES, LANES), LANES)
        there = pl.ds(pl.multiple_of((t + 1) * LANES, LANES), LANES)
        flat = None
        for k in range(2 * nz + 2):
            at = k * (bc + 1)
            piece = jnp.where(
                lane < first + bc + 1 - (t + 1) * LANES, kept[k, :, there], kept[k, :, here]
            )
            piece = pltpu.roll(piece, lax.rem(at + nx - first, LANES), 1)
            flat = piece if flat is None else jnp.where(lane >= at, piece, flat)
        flat = jnp.where(lane < (2 * nz + 2) * (bc + 1), flat, 0.0)
        extra = jnp.concatenate(
            [roll(flat, nz * bf - i * spare, 1) for i in range(rf // yc)], axis=0
        )
        blocks[step] = jnp.where(wide >= nz * bf, extra, tile)

    def block_copy(step):
        g = target(step)
        return remote(blocks.at[step], pencil.at[s], blk_s.at[step], blk_r.at[s], h, g)

    def send(step):
        g = target(step)

        @pl.when(g > s)
        def _():
            pl.semaphore_wait(ready.at[g], 1)

        block_copy(step).start()

    def several(i):
        for j in range(TURN):
            build(TURN * i + j + 1)
        for j in range(TURN):
            send(TURN * i + j + 1)

    turns = (gy - 1) // TURN
    each(0, turns, several)
    for step in range(turns * TURN + 1, gy):
        build(step)
    build(0)
    for step in range(turns * TURN + 1, gy):
        send(step)
    pltpu.make_async_copy(blocks.at[0], pencil.at[s], blk_r.at[s]).start()

    for load in loads[4:]:
        load.wait()
    chunks = ny // LANES
    order = [k % chunks for chunk, width in windows(chunks) for k in range(chunk, chunk + width)]
    here = set()
    below, above = wrapped(h + gz - 1, gz), wrapped(h + 1, gz)
    ups, downs = {}, {}
    for i, (chunk, width) in enumerate(windows(chunks)):
        low, high = touched(chunk, width, yc)
        gs = [g % gy for g in range(low, high + 1)]
        for g in gs:
            if g not in here:
                here.add(g)
                pltpu.make_async_copy(pencil.at[g], pencil.at[g], blk_r.at[g]).wait()
        got = jnp.concatenate([pencil[g] for g in gs], axis=0)
        coarse = [
            jnp.concatenate([pencil[g, at : at + yc, :] for g in gs], axis=0)
            for at in range(0, rf, yc)
        ]
        coarse = jnp.concatenate(coarse, axis=1)
        span = -(-len(gs) // 8) * 8
        if len(gs) < span:
            coarse = jnp.concatenate(
                [coarse, jnp.zeros(((span - len(gs)) * yc, coarse.shape[1]), jnp.float32)], axis=0
            )
        for_y = exact_right(coarse, yy_m[...])
        for_z = exact_left(zz_m[...], coarse, ((1,), (1,)))
        count = width * LANES
        speed_y = exact_left(eyt_m[i, : count + 2 * EDGE, : span * yc], for_y) * NINTH
        speed_zs = exact_right(for_z, ey_m[i, : span * yc, :count]) * NINTH
        start = chunk * LANES - EDGE - low * rf
        swept = sweep_periodic(got[start : start + count + 2 * EDGE], speed_y, 0)
        for j in range(width):
            k = (chunk + j) % chunks
            cols = slice(k * LANES, (k + 1) * LANES)
            speed_z = speed_zs[:, j * LANES : (j + 1) * LANES]
            at = EDGE + j * LANES
            part = jnp.transpose(swept[at : at + LANES])[: nz * bf]
            moved = displacement(
                speed_z[bf : (nz + 1) * bf], speed_z[: nz * bf], speed_z[2 * bf :]
            )
            w = weights(moved)

            def landing(target):
                result = None
                for m in range(-3, 4):
                    z = target - m
                    if 0 <= z < nz:
                        at = slice(z * bf, (z + 1) * bf)
                        term = part[at] * w[m][at]
                        result = term if result is None else result + term
                return result

            for t in range(3):
                up_out[k, t] = landing(nz + t)
                down_out[k, t] = landing(t - 3)
            for t in range(nz):
                out[t, :, cols] = landing(t)
            ups[k] = remote(up_out.at[k], up_in.at[k], z_s.at[0, k], z_r.at[0, k], above, s)
            downs[k] = remote(down_out.at[k], down_in.at[k], z_s.at[1, k], z_r.at[1, k], below, s)

        @pl.when(h < gz - 1)
        def _():
            for j in range(width):
                ups[(chunk + j) % chunks].start()

        @pl.when(h > 0)
        def _():
            for j in range(width):
                downs[(chunk + j) % chunks].start()

    for copy in firsts[1:] + nexts + others[1:]:
        copy.wait_send()
    each(1, gy, lambda step: block_copy(step).wait_send())

    for k in order:
        cols = slice(k * LANES, (k + 1) * LANES)

        @pl.when(h > 0)
        def _():
            ups[k].wait_recv()
            for i in range(3):
                out[i, :, cols] = out[i, :, cols] + up_in[k, i]

        @pl.when(h < gz - 1)
        def _():
            downs[k].wait_recv()
            for i in range(nz - 3, nz):
                out[i, :, cols] = out[i, :, cols] + down_in[k, i - nz + 3]

    @pl.when(h > 0)
    def _():
        for copy in downs.values():
            copy.wait_send()

    @pl.when(h < gz - 1)
    def _():
        for copy in ups.values():
            copy.wait_send()


def local(scalar, velocity):
    gz, gy = lax.axis_size("gz"), lax.axis_size("gy")
    nz, rf, nx = scalar.shape
    yc, xc = velocity.shape[2:]
    bc = gz * xc // gy
    bf = 3 * bc
    ny = gy * rf
    mats = [jnp.asarray(m, jnp.bfloat16) for m in constants(nz, gz, gy, yc, xc)]
    turned = jnp.transpose(velocity, (0, 2, 3, 1))
    f32 = jnp.float32
    dma = pltpu.SemaphoreType.DMA
    anywhere = pl.BlockSpec(memory_space=pl.ANY)
    vmem = pl.BlockSpec(memory_space=pltpu.VMEM)
    scratch = [pltpu.VMEM(scalar.shape, f32), pltpu.VMEM(turned.shape, f32)]
    scratch += [pltpu.VMEM(m.shape, jnp.bfloat16) for m in mats]
    scratch += [
        pltpu.VMEM((gz, nz, LANES), f32),
        pltpu.VMEM((gz, 1, LANES), f32),
        pltpu.VMEM((gz, 2 * nz + 2, LANES), f32),
        pltpu.VMEM((gz, nz, LANES), f32),
        pltpu.VMEM((gz, 1, LANES), f32),
        pltpu.VMEM((gz, 2 * nz + 2, LANES), f32),
        pltpu.VMEM((2 * nz + 2, yc, gz * xc + LANES), f32),
        pltpu.VMEM((gy, rf, LANES), f32),
        pltpu.VMEM((gy, rf, LANES), f32),
    ]
    scratch += [pltpu.VMEM((ny // LANES, 3, bf, LANES), f32)] * 4
    scratch += [dma((n,)) for n in (2 + len(mats), gz, gz, gz, gz, gz, gz, gy, gy)]
    scratch += [dma((2, ny // LANES))] * 2
    scratch += [pltpu.SemaphoreType.REGULAR((gy,))]
    return pl.pallas_call(
        functools.partial(kernel, gz, gy, nz, yc, xc),
        out_shape=pltpu.VMEM((nz, bf, ny), f32),
        in_specs=[anywhere] * (2 + len(mats)),
        out_specs=vmem,
        scratch_shapes=scratch,
        compiler_params=pltpu.CompilerParams(has_side_effects=True, collective_id=0),
    )(scalar, turned, *mats)


def solution(mesh):
    in_specs = (P("gz", "gy", None), P(None, None, "gy", "gz"))
    out_specs = P("gz", "gy", None)
    return jax.shard_map(local, mesh=mesh, in_specs=in_specs, out_specs=out_specs, check_vma=False)
```

```python
import functools

import jax
import jax.numpy as jnp
import numpy as np
from jax import lax
from jax.experimental import pallas as pl
from jax.experimental.pallas import tpu as pltpu
from jax.sharding import PartitionSpec as P

LANES = 128
OUTER = [18.0, -153.0 / 4.0, 255.0 / 8.0, -313.0 / 24.0, 21.0 / 8.0, -5.0 / 24.0]


def shifted(factors, base, slope):
    total = np.polynomial.Polynomial([0.0])
    for factor in reversed(factors):
        total = total * np.polynomial.Polynomial([base, slope]) + factor
    coefs = np.zeros(6)
    coefs[: len(total.coef)] = total.coef
    return [0.0 if abs(c) < 1e-10 else float(c) for c in coefs]


OUTERMOST = shifted(OUTER, 3.0, -1.0)


def horner(factors, value):
    lowest = 0
    while factors[lowest] == 0.0:
        lowest += 1
    result = jnp.full_like(value, factors[-1])
    for factor in reversed(factors[lowest:-1]):
        result = result * value
        if factor != 0.0:
            result = result + factor
    for _ in range(lowest):
        result = result * value
    return result


def weights(moved):
    positive = moved >= 0.0
    square = moved * moved
    last = horner(OUTERMOST, jnp.abs(moved))
    five, ten = 5.0 * last, 10.0 * last
    inner, outer = square - 1.0, square - 4.0
    near = moved * outer * (-1.0 / 6.0)
    far = moved * inner * (1.0 / 24.0)
    near_even, far_even, far_odd = near * moved, far * moved, far + far
    return {
        0: inner * outer * 0.25 - ten,
        1: near_even + near + jnp.where(positive, ten, five),
        -1: near_even - near + jnp.where(positive, five, ten),
        2: far_even + far_odd - jnp.where(positive, five, last),
        -2: far_even - far_odd - jnp.where(positive, last, five),
        3: jnp.where(positive, last, 0.0),
        -3: jnp.where(positive, 0.0, last),
    }


def displacement(speed, before, after):
    return speed + 0.5 * speed * jnp.where(speed >= 0.0, after - speed, speed - before)


def roll(value, shift, axis):
    return pltpu.roll(value, shift % value.shape[axis], axis)


def sweep_periodic(field, speed, axis):
    moved = displacement(speed, roll(speed, 1, axis), roll(speed, -1, axis))
    w = weights(moved)
    result = field * w[0]
    for m in (-3, -2, -1, 1, 2, 3):
        result = result + roll(field * w[m], m, axis)
    return result


def split(value):
    high = value.astype(jnp.bfloat16)
    return high, (value - high.astype(jnp.float32)).astype(jnp.bfloat16)


def dot(a, b, dims=((1,), (0,))):
    return lax.dot_general(a, b, (dims, ((), ())), preferred_element_type=jnp.float32)


def exact_left(a, value, dims=((1,), (0,))):
    high, low = split(value)
    return dot(a, high, dims) + dot(a, low, dims)


def exact_right(value, b):
    high, low = split(value)
    return dot(high, b) + dot(low, b)


EDGE = 8
REACH = 4
SPAN = 24
TURN = 4
WIDTHS = (1, 1, 1, 3)


def windows(chunks):
    out, at = [], 1
    while at <= chunks:
        width = min(WIDTHS[len(out) % len(WIDTHS)], chunks + 1 - at)
        out.append((at, width))
        at += width
    return out


def touched(chunk, width, yc):
    first, end = chunk * LANES, (chunk + width) * LANES
    low = min(((first - REACH) // 3) // yc, (first - EDGE) // (3 * yc))
    high = max(((end + REACH - 1) // 3 + 1) // yc, (end + EDGE - 1) // (3 * yc))
    assert high - low < SPAN
    return low, high


NINTH = 1.0 / 9.0


def along(count):
    out = np.zeros((count, 3 * count), np.float32)
    for c in range(count):
        for k in range(3):
            out[c, 3 * c + k] += 3 - k
            out[(c + 1) % count, 3 * c + k] += k
    return out


def constants(nz, gz, gy, yc, xc):
    bc = gz * xc // gy
    bf = 3 * bc
    rf = 3 * yc
    spare = LANES - nz * bf
    rows = np.zeros((nz * rf, nz * yc + 8), np.float32)
    for z in range(nz):
        for r in range(rf):
            y, k = divmod(r, 3)
            rows[z * rf + r, z * yc + y] += 3 - k
            rows[z * rf + r, z * yc + y + 1 if y < yc - 1 else nz * yc + z] += k
    groups = rf // yc
    to_y = np.zeros((groups * LANES, LANES), np.float32)
    to_z = np.zeros(((nz + 2) * bf, groups * LANES), np.float32)
    for plane in range(2 * nz + 2):
        for c in range(bf):
            for col, weight in ((c // 3, 3 - c % 3), (c // 3 + 1, c % 3)):
                if weight == 0:
                    continue
                group, at = divmod(plane * (bc + 1) + col, spare)
                src = group * LANES + nz * bf + at
                if plane < nz:
                    to_y[src, plane * bf + c] += weight
                else:
                    to_z[(plane - nz) * bf + c, src] += weight
    parts = windows(gy * rf // LANES)
    most = LANES * max(width for _, width in parts)
    down = np.zeros((len(parts), most + 2 * EDGE, SPAN * yc), np.float32)
    across = np.zeros((len(parts), SPAN * yc, most), np.float32)
    for i, (chunk, width) in enumerate(parts):
        base = yc * touched(chunk, width, yc)[0]
        for r in range(-REACH, width * LANES + REACH):
            c, k = divmod(chunk * LANES + r, 3)
            for at, weight in ((c - base, 3 - k), (c + 1 - base, k)):
                if weight:
                    down[i, EDGE + r, at] += weight
                    if 0 <= r < width * LANES:
                        across[i, at, r] += weight
    return rows, along(gz * xc), to_y, to_z, across, down


def wrapped(index, size):
    return jnp.where(index >= size, index - size, index)


def kernel(gz, gy, nz, yc, xc, *refs):
    (scalar_hbm, vel_hbm, rows_hbm, ex_hbm, yy_hbm, zz_hbm, ey_hbm, eyt_hbm, out,
     scalar, vel, rows_m, ex_m, yy_m, zz_m, ey_m, eyt_m,
     xsend, nsend, wsend, own, nxt, other, kept, blocks, pencil,
     up_out, down_out, up_in, down_in,
     local_sem, own_s, own_r, nxt_s, nxt_r, oth_s, oth_r, blk_s, blk_r, z_s, z_r, ready) = refs
    h = lax.axis_index("gz")
    s = lax.axis_index("gy")
    rf = 3 * yc
    bc = gz * xc // gy
    bf = 3 * bc
    total = gz * nz
    nx = scalar.shape[2]
    ny = gy * rf
    behind, ahead = wrapped(s + gy - 1, gy), wrapped(s + 1, gy)

    loads = []
    for i, (src, dst) in enumerate((
        (vel_hbm, vel), (scalar_hbm, scalar), (rows_hbm, rows_m), (ex_hbm, ex_m),
        (yy_hbm, yy_m), (zz_hbm, zz_m), (ey_hbm, ey_m), (eyt_hbm, eyt_m),
    )):
        load = pltpu.make_async_copy(src, dst, local_sem.at[i])
        load.start()
        loads.append(load)

    barrier = pltpu.get_barrier_semaphore()

    def tell(semaphore, p, g):
        pl.semaphore_signal(
            semaphore, inc=1, device_id={"gz": p, "gy": g}, device_id_type=pl.DeviceIdType.MESH
        )

    def each(low, high, act):
        def one(i, _):
            act(i)
            return 0

        lax.fori_loop(low, high, one, 0)

    for step in range(1, gz):
        tell(barrier, wrapped(h + step, gz), s)
    for step in range(gz):
        tell(barrier, wrapped(h + step, gz), ahead)
    each(s + 1, gy, lambda g: tell(barrier, h, g))

    def remote(src, dst, send, recv, p, g):
        return pltpu.make_async_remote_copy(
            src_ref=src, dst_ref=dst, send_sem=send, recv_sem=recv,
            device_id={"gz": p, "gy": g}, device_id_type=pl.DeviceIdType.MESH,
        )

    loads[0].wait()
    fill = jnp.zeros((yc * xc, LANES - total), jnp.float32)

    def by_plane(c):
        wide = jnp.concatenate([vel[c].reshape(yc * xc, total), fill], axis=1)
        return jnp.transpose(wide)

    planes = by_plane(0)
    for p in range(gz):
        xsend[p] = planes[p * nz : (p + 1) * nz]
    tall = lax.broadcasted_iota(jnp.int32, (LANES, LANES), 0)
    bottom = jnp.where(lax.broadcasted_iota(jnp.int32, (LANES, LANES), 1) < xc, planes, 0.0)
    shifts = [roll(bottom, i * xc, 1) if i else bottom for i in range(nz)]
    bottom = shifts[0]
    for i in range(1, nz):
        bottom = jnp.where(tall % nz == i, shifts[i], bottom)
    for p in range(gz):
        nsend[p] = jnp.sum(bottom[p * nz : (p + 1) * nz], axis=0, keepdims=True)
    planes = by_plane(1)
    for p in range(gz):
        wsend[p, :nz] = planes[p * nz : (p + 1) * nz]
    planes = by_plane(2)
    for p in range(gz):
        if p == 0:
            wsend[p, nz : nz + 1] = jnp.zeros((1, LANES), jnp.float32)
            wsend[p, nz + 1 :] = planes[: nz + 1]
        else:
            wsend[p, nz:] = planes[p * nz - 1 : (p + 1) * nz + 1]

    pl.semaphore_wait(barrier, 2 * gz - 1 + s)

    firsts, nexts, others = [], [], []
    for step in range(gz):
        p = wrapped(h + step, gz)
        if step:
            firsts.append(remote(xsend.at[p], own.at[h], own_s.at[step], own_r.at[h], p, s))
            others.append(remote(wsend.at[p], other.at[h], oth_s.at[step], oth_r.at[h], p, s))
        else:
            firsts.append(pltpu.make_async_copy(xsend.at[p], own.at[h], own_r.at[h]))
            others.append(pltpu.make_async_copy(wsend.at[p], other.at[h], oth_r.at[h]))
        nexts.append(remote(nsend.at[p], nxt.at[h], nxt_s.at[step], nxt_r.at[h], p, behind))
    for copy in firsts + nexts + others:
        copy.start()
    each(0, s, lambda g: tell(ready.at[s], h, g))

    lane = lax.broadcasted_iota(jnp.int32, (yc, LANES), 1)
    row = lax.broadcasted_iota(jnp.int32, (yc, LANES), 0)
    block = lane // xc

    def swap(value):
        for k in (1, 2, 4):
            row_bit, lane_bit = (row // k) % 2, (block // k) % 2
            value = jnp.where(
                row_bit == lane_bit,
                value,
                jnp.where(
                    row_bit == 0,
                    roll(roll(value, -k, 0), k * xc, 1),
                    roll(roll(value, k, 0), -k * xc, 1),
                ),
            )
        return value

    halves = [slice(i, i + yc) for i in range(0, gz, yc)]
    for i in range(gz):
        pltpu.make_async_copy(own.at[i], own.at[i], own_r.at[i]).wait()
        pltpu.make_async_copy(nxt.at[i], nxt.at[i], nxt_r.at[i]).wait()
    coarse = []
    for value in [own[:, z, :] for z in range(nz)] + [nxt[:, 0, :]]:
        coarse.append(jnp.concatenate([swap(value[half]) for half in halves], axis=1))
    coarse = jnp.concatenate(coarse, axis=0)
    for load in loads[1:4]:
        load.wait()
    speed = exact_right(exact_left(rows_m[...], coarse), ex_m[...]) * NINTH
    field = scalar[...].reshape(nz * rf, nx)
    field = sweep_periodic(field, speed, 1)
    for z in range(nz):
        plane = field[z * rf : (z + 1) * rf]
        scalar[z] = roll(plane, z * bf, 1) if z else plane

    for i in range(gz):
        pltpu.make_async_copy(other.at[i], other.at[i], oth_r.at[i]).wait()
    for k in range(2 * nz + 2):
        parts = [swap(other[:, k, :][half]) for half in halves]
        row_of = jnp.concatenate(parts, axis=1)
        kept[k] = roll(row_of, k * (bc + 1), 1) if k else row_of
    spare = LANES - nz * bf

    def place(first, count):
        t = lax.div(first, LANES)
        off = first - t * LANES
        tiles = [
            pl.ds(pl.multiple_of(lax.rem(t + i, count) * LANES, LANES), LANES) for i in range(2)
        ]
        return tiles, off, jnp.where(lane < off, lane - off + LANES, lane - off)

    def target(step):
        some = gy // 8
        near = jnp.where(step <= s, s - step, step)
        late = jnp.where(step <= s, s + some - step, step)
        late = jnp.where(step <= some, lax.rem(s + step, some), late)
        return jnp.where((s >= gy // 2) & (step > 0), late, near)

    def build(step):
        g = target(step)
        (here, there), off, at = place(g * bf, nx // LANES)
        (kept_here, kept_there), kept_off, kept_at = place(g * bc, gz * xc // LANES)
        flat = None
        for k in range(2 * nz + 2):
            piece = jnp.where(lane < kept_off, kept[k, :, kept_there], kept[k, :, kept_here])
            flat = piece if flat is None else jnp.where(kept_at >= k * (bc + 1), piece, flat)
        flat = jnp.where(kept_at < (2 * nz + 2) * (bc + 1), flat, 0.0)
        for i in range(rf // yc):
            rows = slice(i * yc, (i + 1) * yc)
            tile = None
            for z in range(nz):
                piece = jnp.where(lane < off, scalar[z, rows, there], scalar[z, rows, here])
                tile = piece if tile is None else jnp.where(at >= z * bf, piece, tile)
            tile = pltpu.roll(tile, lax.rem(LANES - off, LANES), 1)
            extra = pltpu.roll(flat, lax.rem(LANES + nz * bf - i * spare - kept_off, LANES), 1)
            blocks[step, rows] = jnp.where(lane >= nz * bf, extra, tile)

    def block_copy(step):
        g = target(step)
        return remote(blocks.at[step], pencil.at[s], blk_s.at[step], blk_r.at[s], h, g)

    def send(step):
        g = target(step)

        @pl.when(g > s)
        def _():
            pl.semaphore_wait(ready.at[g], 1)

        block_copy(step).start()

    def several(i):
        for j in range(TURN):
            build(TURN * i + j + 1)
        for j in range(TURN):
            send(TURN * i + j + 1)

    turns = (gy - 1) // TURN
    each(0, turns, several)
    for step in range(turns * TURN + 1, gy):
        build(step)
    build(0)
    for step in range(turns * TURN + 1, gy):
        send(step)
    pltpu.make_async_copy(blocks.at[0], pencil.at[s], blk_r.at[s]).start()

    for load in loads[4:]:
        load.wait()
    chunks = ny // LANES
    order = [k % chunks for chunk, width in windows(chunks) for k in range(chunk, chunk + width)]
    here = set()
    below, above = wrapped(h + gz - 1, gz), wrapped(h + 1, gz)
    ups, downs = {}, {}
    for i, (chunk, width) in enumerate(windows(chunks)):
        low, high = touched(chunk, width, yc)
        gs = [g % gy for g in range(low, high + 1)]
        for g in gs:
            if g not in here:
                here.add(g)
                pltpu.make_async_copy(pencil.at[g], pencil.at[g], blk_r.at[g]).wait()
        got = jnp.concatenate([pencil[g] for g in gs], axis=0)
        coarse = [
            jnp.concatenate([pencil[g, at : at + yc, :] for g in gs], axis=0)
            for at in range(0, rf, yc)
        ]
        coarse = jnp.concatenate(coarse, axis=1)
        span = -(-len(gs) // 8) * 8
        if len(gs) < span:
            coarse = jnp.concatenate(
                [coarse, jnp.zeros(((span - len(gs)) * yc, coarse.shape[1]), jnp.float32)], axis=0
            )
        for_y = exact_right(coarse, yy_m[...])
        for_z = exact_left(zz_m[...], coarse, ((1,), (1,)))
        count = width * LANES
        speed_y = exact_left(eyt_m[i, : count + 2 * EDGE, : span * yc], for_y) * NINTH
        speed_zs = exact_right(for_z, ey_m[i, : span * yc, :count]) * NINTH
        start = chunk * LANES - EDGE - low * rf
        swept = sweep_periodic(got[start : start + count + 2 * EDGE], speed_y, 0)
        for j in range(width):
            k = (chunk + j) % chunks
            cols = slice(k * LANES, (k + 1) * LANES)
            speed_z = speed_zs[:, j * LANES : (j + 1) * LANES]
            at = EDGE + j * LANES
            part = jnp.transpose(swept[at : at + LANES])[: nz * bf]
            moved = displacement(
                speed_z[bf : (nz + 1) * bf], speed_z[: nz * bf], speed_z[2 * bf :]
            )
            w = weights(moved)

            def landing(target):
                result = None
                for m in range(-3, 4):
                    z = target - m
                    if 0 <= z < nz:
                        at = slice(z * bf, (z + 1) * bf)
                        term = part[at] * w[m][at]
                        result = term if result is None else result + term
                return result

            for t in range(3):
                up_out[k, t] = landing(nz + t)
                down_out[k, t] = landing(t - 3)
            for t in range(nz):
                out[t, :, cols] = landing(t)
            ups[k] = remote(up_out.at[k], up_in.at[k], z_s.at[0, k], z_r.at[0, k], above, s)
            downs[k] = remote(down_out.at[k], down_in.at[k], z_s.at[1, k], z_r.at[1, k], below, s)

        @pl.when(h < gz - 1)
        def _():
            for j in range(width):
                ups[(chunk + j) % chunks].start()

        @pl.when(h > 0)
        def _():
            for j in range(width):
                downs[(chunk + j) % chunks].start()

    for copy in firsts[1:] + nexts + others[1:]:
        copy.wait_send()
    each(1, gy, lambda step: block_copy(step).wait_send())

    for k in order:
        cols = slice(k * LANES, (k + 1) * LANES)

        @pl.when(h > 0)
        def _():
            ups[k].wait_recv()
            for i in range(3):
                out[i, :, cols] = out[i, :, cols] + up_in[k, i]

        @pl.when(h < gz - 1)
        def _():
            downs[k].wait_recv()
            for i in range(nz - 3, nz):
                out[i, :, cols] = out[i, :, cols] + down_in[k, i - nz + 3]

    @pl.when(h > 0)
    def _():
        for copy in downs.values():
            copy.wait_send()

    @pl.when(h < gz - 1)
    def _():
        for copy in ups.values():
            copy.wait_send()


def local(scalar, velocity):
    gz, gy = lax.axis_size("gz"), lax.axis_size("gy")
    nz, rf, nx = scalar.shape
    yc, xc = velocity.shape[2:]
    bc = gz * xc // gy
    bf = 3 * bc
    ny = gy * rf
    mats = [jnp.asarray(m, jnp.bfloat16) for m in constants(nz, gz, gy, yc, xc)]
    turned = jnp.transpose(velocity, (0, 2, 3, 1))
    f32 = jnp.float32
    dma = pltpu.SemaphoreType.DMA
    anywhere = pl.BlockSpec(memory_space=pl.ANY)
    vmem = pl.BlockSpec(memory_space=pltpu.VMEM)
    scratch = [pltpu.VMEM(scalar.shape, f32), pltpu.VMEM(turned.shape, f32)]
    scratch += [pltpu.VMEM(m.shape, jnp.bfloat16) for m in mats]
    scratch += [
        pltpu.VMEM((gz, nz, LANES), f32),
        pltpu.VMEM((gz, 1, LANES), f32),
        pltpu.VMEM((gz, 2 * nz + 2, LANES), f32),
        pltpu.VMEM((gz, nz, LANES), f32),
        pltpu.VMEM((gz, 1, LANES), f32),
        pltpu.VMEM((gz, 2 * nz + 2, LANES), f32),
        pltpu.VMEM((2 * nz + 2, yc, gz * xc), f32),
        pltpu.VMEM((gy, rf, LANES), f32),
        pltpu.VMEM((gy, rf, LANES), f32),
    ]
    scratch += [pltpu.VMEM((ny // LANES, 3, bf, LANES), f32)] * 4
    scratch += [dma((n,)) for n in (2 + len(mats), gz, gz, gz, gz, gz, gz, gy, gy)]
    scratch += [dma((2, ny // LANES))] * 2
    scratch += [pltpu.SemaphoreType.REGULAR((gy,))]
    return pl.pallas_call(
        functools.partial(kernel, gz, gy, nz, yc, xc),
        out_shape=pltpu.VMEM((nz, bf, ny), f32),
        in_specs=[anywhere] * (2 + len(mats)),
        out_specs=vmem,
        scratch_shapes=scratch,
        compiler_params=pltpu.CompilerParams(has_side_effects=True, collective_id=0),
    )(scalar, turned, *mats)


def solution(mesh):
    in_specs = (P("gz", "gy", None), P(None, None, "gy", "gz"))
    out_specs = P("gz", "gy", None)
    return jax.shard_map(local, mesh=mesh, in_specs=in_specs, out_specs=out_specs, check_vma=False)
```

```python
import functools

import jax
import jax.numpy as jnp
import numpy as np
from jax import lax
from jax.experimental import pallas as pl
from jax.experimental.pallas import tpu as pltpu
from jax.sharding import PartitionSpec as P

LANES = 128
OUTER = [18.0, -153.0 / 4.0, 255.0 / 8.0, -313.0 / 24.0, 21.0 / 8.0, -5.0 / 24.0]


def shifted(factors, base, slope):
    total = np.polynomial.Polynomial([0.0])
    for factor in reversed(factors):
        total = total * np.polynomial.Polynomial([base, slope]) + factor
    coefs = np.zeros(6)
    coefs[: len(total.coef)] = total.coef
    return [0.0 if abs(c) < 1e-10 else float(c) for c in coefs]


OUTERMOST = shifted(OUTER, 3.0, -1.0)


def horner(factors, value):
    lowest = 0
    while factors[lowest] == 0.0:
        lowest += 1
    result = jnp.full_like(value, factors[-1])
    for factor in reversed(factors[lowest:-1]):
        result = result * value
        if factor != 0.0:
            result = result + factor
    for _ in range(lowest):
        result = result * value
    return result


def weights(moved):
    positive = moved >= 0.0
    square = moved * moved
    last = horner(OUTERMOST, jnp.abs(moved))
    five, ten = 5.0 * last, 10.0 * last
    inner, outer = square - 1.0, square - 4.0
    near = moved * outer * (-1.0 / 6.0)
    far = moved * inner * (1.0 / 24.0)
    near_even, far_even, far_odd = near * moved, far * moved, far + far
    return {
        0: inner * outer * 0.25 - ten,
        1: near_even + near + jnp.where(positive, ten, five),
        -1: near_even - near + jnp.where(positive, five, ten),
        2: far_even + far_odd - jnp.where(positive, five, last),
        -2: far_even - far_odd - jnp.where(positive, last, five),
        3: jnp.where(positive, last, 0.0),
        -3: jnp.where(positive, 0.0, last),
    }


def displacement(speed, before, after):
    return speed + 0.5 * speed * jnp.where(speed >= 0.0, after - speed, speed - before)


def roll(value, shift, axis):
    return pltpu.roll(value, shift % value.shape[axis], axis)


def sweep_periodic(field, speed, axis):
    moved = displacement(speed, roll(speed, 1, axis), roll(speed, -1, axis))
    w = weights(moved)
    result = field * w[0]
    for m in (-3, -2, -1, 1, 2, 3):
        result = result + roll(field * w[m], m, axis)
    return result


def split(value):
    high = value.astype(jnp.bfloat16)
    return high, (value - high.astype(jnp.float32)).astype(jnp.bfloat16)


def dot(a, b, dims=((1,), (0,))):
    return lax.dot_general(a, b, (dims, ((), ())), preferred_element_type=jnp.float32)


def exact_left(a, value, dims=((1,), (0,))):
    high, low = split(value)
    return dot(a, high, dims) + dot(a, low, dims)


def exact_right(value, b):
    high, low = split(value)
    return dot(high, b) + dot(low, b)


EDGE = 8
REACH = 4
SPAN = 16
TURN = 4
WIDTHS = (1, 1, 1, 1, 2)


def windows(chunks):
    out, at = [], 1
    while at <= chunks:
        width = min(WIDTHS[len(out) % len(WIDTHS)], chunks + 1 - at)
        out.append((at, width))
        at += width
    return out


def touched(chunk, width, yc):
    first, end = chunk * LANES, (chunk + width) * LANES
    low = min(((first - REACH) // 3) // yc, (first - EDGE) // (3 * yc))
    high = max(((end + REACH - 1) // 3 + 1) // yc, (end + EDGE - 1) // (3 * yc))
    assert high - low < SPAN
    return low, high


NINTH = 1.0 / 9.0


def along(count):
    out = np.zeros((count, 3 * count), np.float32)
    for c in range(count):
        for k in range(3):
            out[c, 3 * c + k] += 3 - k
            out[(c + 1) % count, 3 * c + k] += k
    return out


def constants(nz, gz, gy, yc, xc):
    bc = gz * xc // gy
    bf = 3 * bc
    rf = 3 * yc
    spare = LANES - nz * bf
    rows = np.zeros((nz * rf, nz * yc + 8), np.float32)
    for z in range(nz):
        for r in range(rf):
            y, k = divmod(r, 3)
            rows[z * rf + r, z * yc + y] += 3 - k
            rows[z * rf + r, z * yc + y + 1 if y < yc - 1 else nz * yc + z] += k
    groups = rf // yc
    to_y = np.zeros((groups * LANES, LANES), np.float32)
    to_z = np.zeros(((nz + 2) * bf, groups * LANES), np.float32)
    for plane in range(2 * nz + 2):
        for c in range(bf):
            for col, weight in ((c // 3, 3 - c % 3), (c // 3 + 1, c % 3)):
                if weight == 0:
                    continue
                group, at = divmod(plane * (bc + 1) + col, spare)
                src = group * LANES + nz * bf + at
                if plane < nz:
                    to_y[src, plane * bf + c] += weight
                else:
                    to_z[(plane - nz) * bf + c, src] += weight
    parts = windows(gy * rf // LANES)
    most = LANES * max(width for _, width in parts)
    down = np.zeros((len(parts), most + 2 * EDGE, SPAN * yc), np.float32)
    across = np.zeros((len(parts), SPAN * yc, most), np.float32)
    for i, (chunk, width) in enumerate(parts):
        base = yc * touched(chunk, width, yc)[0]
        for r in range(-REACH, width * LANES + REACH):
            c, k = divmod(chunk * LANES + r, 3)
            for at, weight in ((c - base, 3 - k), (c + 1 - base, k)):
                if weight:
                    down[i, EDGE + r, at] += weight
                    if 0 <= r < width * LANES:
                        across[i, at, r] += weight
    return rows, along(gz * xc), to_y, to_z, across, down


def wrapped(index, size):
    return jnp.where(index >= size, index - size, index)


def kernel(gz, gy, nz, yc, xc, *refs):
    (scalar_hbm, vel_hbm, rows_hbm, ex_hbm, yy_hbm, zz_hbm, ey_hbm, eyt_hbm, out,
     scalar, vel, rows_m, ex_m, yy_m, zz_m, ey_m, eyt_m,
     xsend, nsend, wsend, own, nxt, other, kept, blocks, pencil,
     up_out, down_out, up_in, down_in,
     local_sem, own_s, own_r, nxt_s, nxt_r, oth_s, oth_r, blk_s, blk_r, z_s, z_r, ready) = refs
    h = lax.axis_index("gz")
    s = lax.axis_index("gy")
    rf = 3 * yc
    bc = gz * xc // gy
    bf = 3 * bc
    total = gz * nz
    nx = scalar.shape[2]
    ny = gy * rf
    behind, ahead = wrapped(s + gy - 1, gy), wrapped(s + 1, gy)

    loads = []
    for i, (src, dst) in enumerate((
        (vel_hbm, vel), (scalar_hbm, scalar), (rows_hbm, rows_m), (ex_hbm, ex_m),
        (yy_hbm, yy_m), (zz_hbm, zz_m), (ey_hbm, ey_m), (eyt_hbm, eyt_m),
    )):
        load = pltpu.make_async_copy(src, dst, local_sem.at[i])
        load.start()
        loads.append(load)

    barrier = pltpu.get_barrier_semaphore()

    def tell(semaphore, p, g):
        pl.semaphore_signal(
            semaphore, inc=1, device_id={"gz": p, "gy": g}, device_id_type=pl.DeviceIdType.MESH
        )

    def each(low, high, act):
        def one(i, _):
            act(i)
            return 0

        lax.fori_loop(low, high, one, 0)

    for step in range(1, gz):
        tell(barrier, wrapped(h + step, gz), s)
    for step in range(gz):
        tell(barrier, wrapped(h + step, gz), ahead)
    each(s + 1, gy, lambda g: tell(barrier, h, g))

    def remote(src, dst, send, recv, p, g):
        return pltpu.make_async_remote_copy(
            src_ref=src, dst_ref=dst, send_sem=send, recv_sem=recv,
            device_id={"gz": p, "gy": g}, device_id_type=pl.DeviceIdType.MESH,
        )

    loads[0].wait()
    fill = jnp.zeros((yc * xc, LANES - total), jnp.float32)

    def by_plane(c):
        wide = jnp.concatenate([vel[c].reshape(yc * xc, total), fill], axis=1)
        return jnp.transpose(wide)

    planes = by_plane(0)
    for p in range(gz):
        xsend[p] = planes[p * nz : (p + 1) * nz]
    tall = lax.broadcasted_iota(jnp.int32, (LANES, LANES), 0)
    bottom = jnp.where(lax.broadcasted_iota(jnp.int32, (LANES, LANES), 1) < xc, planes, 0.0)
    shifts = [roll(bottom, i * xc, 1) if i else bottom for i in range(nz)]
    bottom = shifts[0]
    for i in range(1, nz):
        bottom = jnp.where(tall % nz == i, shifts[i], bottom)
    for p in range(gz):
        nsend[p] = jnp.sum(bottom[p * nz : (p + 1) * nz], axis=0, keepdims=True)
    planes = by_plane(1)
    for p in range(gz):
        wsend[p, :nz] = planes[p * nz : (p + 1) * nz]
    planes = by_plane(2)
    for p in range(gz):
        if p == 0:
            wsend[p, nz : nz + 1] = jnp.zeros((1, LANES), jnp.float32)
            wsend[p, nz + 1 :] = planes[: nz + 1]
        else:
            wsend[p, nz:] = planes[p * nz - 1 : (p + 1) * nz + 1]

    pl.semaphore_wait(barrier, 2 * gz - 1 + s)

    firsts, nexts, others = [], [], []
    for step in range(gz):
        p = wrapped(h + step, gz)
        if step:
            firsts.append(remote(xsend.at[p], own.at[h], own_s.at[step], own_r.at[h], p, s))
            others.append(remote(wsend.at[p], other.at[h], oth_s.at[step], oth_r.at[h], p, s))
        else:
            firsts.append(pltpu.make_async_copy(xsend.at[p], own.at[h], own_r.at[h]))
            others.append(pltpu.make_async_copy(wsend.at[p], other.at[h], oth_r.at[h]))
        nexts.append(remote(nsend.at[p], nxt.at[h], nxt_s.at[step], nxt_r.at[h], p, behind))
    for copy in firsts + nexts + others:
        copy.start()
    each(0, s, lambda g: tell(ready.at[s], h, g))

    lane = lax.broadcasted_iota(jnp.int32, (yc, LANES), 1)
    row = lax.broadcasted_iota(jnp.int32, (yc, LANES), 0)
    block = lane // xc

    def swap(value):
        for k in (1, 2, 4):
            row_bit, lane_bit = (row // k) % 2, (block // k) % 2
            value = jnp.where(
                row_bit == lane_bit,
                value,
                jnp.where(
                    row_bit == 0,
                    roll(roll(value, -k, 0), k * xc, 1),
                    roll(roll(value, k, 0), -k * xc, 1),
                ),
            )
        return value

    halves = [slice(i, i + yc) for i in range(0, gz, yc)]
    for i in range(gz):
        pltpu.make_async_copy(own.at[i], own.at[i], own_r.at[i]).wait()
        pltpu.make_async_copy(nxt.at[i], nxt.at[i], nxt_r.at[i]).wait()
    coarse = []
    for value in [own[:, z, :] for z in range(nz)] + [nxt[:, 0, :]]:
        coarse.append(jnp.concatenate([swap(value[half]) for half in halves], axis=1))
    coarse = jnp.concatenate(coarse, axis=0)
    for load in loads[1:4]:
        load.wait()
    speed = exact_right(exact_left(rows_m[...], coarse), ex_m[...]) * NINTH
    field = scalar[...].reshape(nz * rf, nx)
    field = sweep_periodic(field, speed, 1)
    for z in range(nz):
        plane = field[z * rf : (z + 1) * rf]
        scalar[z] = roll(plane, z * bf, 1) if z else plane

    for i in range(gz):
        pltpu.make_async_copy(other.at[i], other.at[i], oth_r.at[i]).wait()
    for k in range(2 * nz + 2):
        parts = [swap(other[:, k, :][half]) for half in halves]
        row_of = jnp.concatenate(parts, axis=1)
        kept[k] = roll(row_of, k * (bc + 1), 1) if k else row_of
    spare = LANES - nz * bf

    def place(first, count):
        t = lax.div(first, LANES)
        off = first - t * LANES
        tiles = [
            pl.ds(pl.multiple_of(lax.rem(t + i, count) * LANES, LANES), LANES) for i in range(2)
        ]
        return tiles, off, jnp.where(lane < off, lane - off + LANES, lane - off)

    def target(step):
        some = gy // 8
        middle = s < 3 * gy // 4
        near = jnp.where(step <= s, s - step, step)
        late = s + some - step
        late = jnp.where(middle & (late < 2 * some), late - some, late)
        late = jnp.where(step <= s, late, step)
        first = jnp.where(middle, some, 0) + lax.rem(s + step, some)
        late = jnp.where(step <= some, first, late)
        return jnp.where((s >= gy // 2) & (step > 0), late, near)

    def build(step):
        g = target(step)
        (here, there), off, at = place(g * bf, nx // LANES)
        (kept_here, kept_there), kept_off, kept_at = place(g * bc, gz * xc // LANES)
        flat = None
        for k in range(2 * nz + 2):
            piece = jnp.where(lane < kept_off, kept[k, :, kept_there], kept[k, :, kept_here])
            flat = piece if flat is None else jnp.where(kept_at >= k * (bc + 1), piece, flat)
        flat = jnp.where(kept_at < (2 * nz + 2) * (bc + 1), flat, 0.0)
        for i in range(rf // yc):
            rows = slice(i * yc, (i + 1) * yc)
            tile = None
            for z in range(nz):
                piece = jnp.where(lane < off, scalar[z, rows, there], scalar[z, rows, here])
                tile = piece if tile is None else jnp.where(at >= z * bf, piece, tile)
            tile = pltpu.roll(tile, lax.rem(LANES - off, LANES), 1)
            extra = pltpu.roll(flat, lax.rem(LANES + nz * bf - i * spare - kept_off, LANES), 1)
            blocks[step, rows] = jnp.where(lane >= nz * bf, extra, tile)

    def block_copy(step):
        g = target(step)
        return remote(blocks.at[step], pencil.at[s], blk_s.at[step], blk_r.at[s], h, g)

    def send(step):
        g = target(step)

        @pl.when(g > s)
        def _():
            pl.semaphore_wait(ready.at[g], 1)

        block_copy(step).start()

    def several(i):
        for j in range(TURN):
            build(TURN * i + j + 1)
        for j in range(TURN):
            send(TURN * i + j + 1)

    turns = (gy - 1) // TURN
    each(0, turns, several)
    for step in range(turns * TURN + 1, gy):
        build(step)
    build(0)
    for step in range(turns * TURN + 1, gy):
        send(step)
    pltpu.make_async_copy(blocks.at[0], pencil.at[s], blk_r.at[s]).start()

    for load in loads[4:]:
        load.wait()
    chunks = ny // LANES
    order = [k % chunks for chunk, width in windows(chunks) for k in range(chunk, chunk + width)]
    here = set()
    below, above = wrapped(h + gz - 1, gz), wrapped(h + 1, gz)
    ups, downs = {}, {}
    for i, (chunk, width) in enumerate(windows(chunks)):
        low, high = touched(chunk, width, yc)
        gs = [g % gy for g in range(low, high + 1)]
        for g in gs:
            if g not in here:
                here.add(g)
                pltpu.make_async_copy(pencil.at[g], pencil.at[g], blk_r.at[g]).wait()
        got = jnp.concatenate([pencil[g] for g in gs], axis=0)
        coarse = [
            jnp.concatenate([pencil[g, at : at + yc, :] for g in gs], axis=0)
            for at in range(0, rf, yc)
        ]
        coarse = jnp.concatenate(coarse, axis=1)
        span = -(-len(gs) // 8) * 8
        if len(gs) < span:
            coarse = jnp.concatenate(
                [coarse, jnp.zeros(((span - len(gs)) * yc, coarse.shape[1]), jnp.float32)], axis=0
            )
        for_y = exact_right(coarse, yy_m[...])
        for_z = exact_left(zz_m[...], coarse, ((1,), (1,)))
        count = width * LANES
        speed_y = exact_left(eyt_m[i, : count + 2 * EDGE, : span * yc], for_y) * NINTH
        speed_zs = exact_right(for_z, ey_m[i, : span * yc, :count]) * NINTH
        start = chunk * LANES - EDGE - low * rf
        swept = sweep_periodic(got[start : start + count + 2 * EDGE], speed_y, 0)
        for j in range(width):
            k = (chunk + j) % chunks
            cols = slice(k * LANES, (k + 1) * LANES)
            speed_z = speed_zs[:, j * LANES : (j + 1) * LANES]
            at = EDGE + j * LANES
            part = jnp.transpose(swept[at : at + LANES])[: nz * bf]
            moved = displacement(
                speed_z[bf : (nz + 1) * bf], speed_z[: nz * bf], speed_z[2 * bf :]
            )
            w = weights(moved)

            def landing(target):
                result = None
                for m in range(-3, 4):
                    z = target - m
                    if 0 <= z < nz:
                        at = slice(z * bf, (z + 1) * bf)
                        term = part[at] * w[m][at]
                        result = term if result is None else result + term
                return result

            for t in range(3):
                up_out[k, t] = landing(nz + t)
                down_out[k, t] = landing(t - 3)
            for t in range(nz):
                out[t, :, cols] = landing(t)
            ups[k] = remote(up_out.at[k], up_in.at[k], z_s.at[0, k], z_r.at[0, k], above, s)
            downs[k] = remote(down_out.at[k], down_in.at[k], z_s.at[1, k], z_r.at[1, k], below, s)

        @pl.when(h < gz - 1)
        def _():
            for j in range(width):
                ups[(chunk + j) % chunks].start()

        @pl.when(h > 0)
        def _():
            for j in range(width):
                downs[(chunk + j) % chunks].start()

    for copy in firsts[1:] + nexts + others[1:]:
        copy.wait_send()
    each(1, gy, lambda step: block_copy(step).wait_send())

    for k in order:
        cols = slice(k * LANES, (k + 1) * LANES)

        @pl.when(h > 0)
        def _():
            ups[k].wait_recv()
            for i in range(3):
                out[i, :, cols] = out[i, :, cols] + up_in[k, i]

        @pl.when(h < gz - 1)
        def _():
            downs[k].wait_recv()
            for i in range(nz - 3, nz):
                out[i, :, cols] = out[i, :, cols] + down_in[k, i - nz + 3]

    @pl.when(h > 0)
    def _():
        for copy in downs.values():
            copy.wait_send()

    @pl.when(h < gz - 1)
    def _():
        for copy in ups.values():
            copy.wait_send()


def local(scalar, velocity):
    gz, gy = lax.axis_size("gz"), lax.axis_size("gy")
    nz, rf, nx = scalar.shape
    yc, xc = velocity.shape[2:]
    bc = gz * xc // gy
    bf = 3 * bc
    ny = gy * rf
    mats = [jnp.asarray(m, jnp.bfloat16) for m in constants(nz, gz, gy, yc, xc)]
    turned = jnp.transpose(velocity, (0, 2, 3, 1))
    f32 = jnp.float32
    dma = pltpu.SemaphoreType.DMA
    anywhere = pl.BlockSpec(memory_space=pl.ANY)
    vmem = pl.BlockSpec(memory_space=pltpu.VMEM)
    scratch = [pltpu.VMEM(scalar.shape, f32), pltpu.VMEM(turned.shape, f32)]
    scratch += [pltpu.VMEM(m.shape, jnp.bfloat16) for m in mats]
    scratch += [
        pltpu.VMEM((gz, nz, LANES), f32),
        pltpu.VMEM((gz, 1, LANES), f32),
        pltpu.VMEM((gz, 2 * nz + 2, LANES), f32),
        pltpu.VMEM((gz, nz, LANES), f32),
        pltpu.VMEM((gz, 1, LANES), f32),
        pltpu.VMEM((gz, 2 * nz + 2, LANES), f32),
        pltpu.VMEM((2 * nz + 2, yc, gz * xc), f32),
        pltpu.VMEM((gy, rf, LANES), f32),
        pltpu.VMEM((gy, rf, LANES), f32),
    ]
    scratch += [pltpu.VMEM((ny // LANES, 3, bf, LANES), f32)] * 4
    scratch += [dma((n,)) for n in (2 + len(mats), gz, gz, gz, gz, gz, gz, gy, gy)]
    scratch += [dma((2, ny // LANES))] * 2
    scratch += [pltpu.SemaphoreType.REGULAR((gy,))]
    return pl.pallas_call(
        functools.partial(kernel, gz, gy, nz, yc, xc),
        out_shape=pltpu.VMEM((nz, bf, ny), f32),
        in_specs=[anywhere] * (2 + len(mats)),
        out_specs=vmem,
        scratch_shapes=scratch,
        compiler_params=pltpu.CompilerParams(has_side_effects=True, collective_id=0),
    )(scalar, turned, *mats)


def solution(mesh):
    in_specs = (P("gz", "gy", None), P(None, None, "gy", "gz"))
    out_specs = P("gz", "gy", None)
    return jax.shard_map(local, mesh=mesh, in_specs=in_specs, out_specs=out_specs, check_vma=False)
```
